32 devices in a mesh: dp: 8 (over z, y), expert: 2 (over core), tensor: 2 (over x).
Axes of the slice: x: 2, y: 2, z: 4, core: 2. Of those that a mesh axis runs over, the one named last changes fastest.
Arguments:
- dense_act: bfloat16 [2, 32, 512, 3584], P(None, 'dp', 'expert', 'tensor'), may hold values from -6 to 6
- dense_cot: bfloat16 [2, 32, 512, 3584], P(None, 'dp', ('expert', 'tensor')), may hold values from -6 to 6
- dense_proj_in: bfloat16 [2, 3584, 128], P(None, 'tensor'), may hold values from -0.09375 to 0.09375
- dense_proj_out: bfloat16 [2, 3584, 128], replicated, may hold values from -0.09375 to 0.09375
- expert_act: bfloat16 [32, 8, 64, 2560], P('dp', 'expert', None, 'tensor'), may hold values from -6 to 6
- expert_cot: bfloat16 [32, 8, 64, 3584], P('dp', 'expert', 'tensor'), may hold values from -6 to 6
- expert_proj_in: bfloat16 [2560, 128], P('tensor'), may hold values from -0.125 to 0.125
- expert_proj_out: bfloat16 [3584, 128], replicated, may hold values from -0.09375 to 0.09375
- dense_valid: float32 [2, 128, 128], replicated, may hold values from -0.0012207031 to 0.0012207031
- expert_valid: float32 [8, 128, 128], P('expert'), may hold values from -0.0012207031 to 0.0012207031
- domain_ids: int32 [32], P('dp'), may hold values from 0 to 63
- prior_mix: float32 [64], replicated, may hold values from 0.002 to 0.05
Outputs:
- log_mixture_weights: float32 [64], P('dp')
The draws below stay inside these ranges and needn't reach their ends.
All inputs are finite; a program needn't handle non-finite values.
Results may differ from the reference program's by a relative error of at most 0.0003.
Values sent between devices are 32-bit elements; how exact they have to be, the bound alone decides.
A program may use at most 128 MiB of HBM per device.

```python
import math
import jax
import jax.numpy as jnp
from jax import lax

D = 3584
FFE = 2560
R = 128
LAYERS = 2
DOMAINS = 64
TOK_MB = 512
CAP = 64
MICRO = 32
EXPERTS = 8


def plant(array, own_key, low, high):
    place = [jax.random.randint(jax.random.fold_in(own_key, axis), (), 0, length) for axis, length in enumerate(array.shape)]
    main_axis = array.shape.index(max(array.shape))
    neighbour = place[:main_axis] + [(place[main_axis] + 1) % array.shape[main_axis]] + place[main_axis + 1:]
    return array.at[tuple(place)].set(low).at[tuple(neighbour)].set(high)


def steps_of(own_key, extent, cuts, smallest, high):
    def one(position, shards_of):
        heights = jax.random.uniform(jax.random.fold_in(jax.random.fold_in(own_key, 6), position), (shards_of,), jnp.float32, smallest / len(cuts), high / len(cuts))
        return jnp.repeat(jnp.exp(heights), extent[position] // shards_of).reshape((-1,) + (1,) * (len(extent) - position - 1))

    loudness = one(*cuts[0])
    for cut in cuts[1:]:
        loudness = loudness * one(*cut)
    return loudness


def gaussian(key, shape, scale, reach, split=(), kind=jnp.bfloat16):
    entries = jax.random.normal(key, shape, jnp.float32) * scale
    if len(split) > 0:
        entries = steps_of(key, shape, split, -0.22, 0.18) * entries
    return jnp.clip(entries, min=-reach, max=reach).astype(kind)


def setup_inputs(seed: int = 0) -> dict:
    key_list = jax.random.split(jax.random.key(seed), 13)
    dense_act = gaussian(key_list[0], (LAYERS, MICRO, TOK_MB, D), 1.0, 6.0, ((1, 8), (2, 2), (3, 2)))
    dense_cot = gaussian(key_list[1], (LAYERS, MICRO, TOK_MB, D), 1.0, 6.0, ((1, 8), (2, 4)))
    dense_proj_in = gaussian(key_list[2], (LAYERS, D, R), D ** -0.5, 0.09375, ((1, 2),))
    dense_proj_out = gaussian(key_list[3], (LAYERS, D, R), D ** -0.5, 0.09375)
    expert_act = gaussian(key_list[4], (MICRO, EXPERTS, CAP, FFE), 1.0, 6.0, ((0, 8), (1, 2), (3, 2)))
    expert_cot = gaussian(key_list[5], (MICRO, EXPERTS, CAP, D), 1.0, 6.0, ((0, 8), (1, 2), (2, 2)))
    expert_proj_in = gaussian(key_list[6], (FFE, R), FFE ** -0.5, 0.125, ((0, 2),))
    expert_proj_out = gaussian(key_list[7], (D, R), D ** -0.5, 0.09375)
    dense_valid = gaussian(key_list[8], (LAYERS, R, R), (R * R * (LAYERS * TOK_MB + EXPERTS * CAP)) ** -0.5, 0.0012207031, (), jnp.float32)
    expert_valid = gaussian(key_list[9], (EXPERTS, R, R), (R * R * (LAYERS * TOK_MB + EXPERTS * CAP)) ** -0.5, 0.0012207031, ((0, 2),), jnp.float32)
    domain_ids = plant(jax.random.randint(key_list[10], (MICRO,), 0, DOMAINS), jax.random.fold_in(key_list[10], 1), 0, DOMAINS - 1).astype(jnp.int32)
    prior_mix = jnp.clip(jnp.exp(jax.random.uniform(key_list[11], (DOMAINS,), jnp.float32, math.log(0.002), math.log(0.05))), 0.002, 0.05)
    return dict(dense_act=dense_act, dense_cot=dense_cot, dense_proj_in=dense_proj_in, dense_proj_out=dense_proj_out, expert_act=expert_act, expert_cot=expert_cot, expert_proj_in=expert_proj_in, expert_proj_out=expert_proj_out, dense_valid=dense_valid, expert_valid=expert_valid, domain_ids=domain_ids, prior_mix=prior_mix)


def reference(dense_act, dense_cot, dense_proj_in, dense_proj_out, expert_act, expert_cot, expert_proj_in, expert_proj_out, dense_valid, expert_valid, domain_ids, prior_mix):
    width = dense_act.shape[3]
    micro = dense_act.shape[1]
    tokens = dense_act.shape[2]
    rank = dense_proj_in.shape[2]
    score = jnp.zeros((micro,), jnp.float32)
    for layer in range(dense_act.shape[0]):
        dense_update_vector = jnp.dot(dense_act[layer].reshape(-1, width), dense_proj_in[layer], preferred_element_type=jnp.float32).reshape(micro, tokens, rank)
        dense_weight_matrix = jnp.dot(dense_cot[layer].reshape(-1, width), dense_proj_out[layer], preferred_element_type=jnp.float32).reshape(micro, tokens, rank)
        sketch = jnp.einsum('mtr,mts->mrs', dense_update_vector, dense_weight_matrix, precision=lax.Precision.HIGHEST)
        score = score + lax.optimization_barrier(jnp.sum(sketch * dense_valid[layer][None], axis=(1, 2)))
    experts = expert_act.shape[1]
    slots = expert_act.shape[2]
    expert_u = jnp.dot(expert_act.reshape(-1, expert_act.shape[3]), expert_proj_in, preferred_element_type=jnp.float32).reshape(micro, experts, slots, rank)
    expert_weight_matrix = jnp.dot(expert_cot.reshape(-1, width), expert_proj_out, preferred_element_type=jnp.float32).reshape(micro, experts, slots, rank)
    expert_sketch = jnp.einsum('mecr,mecs->mers', expert_u, expert_weight_matrix, precision=lax.Precision.HIGHEST)
    score = score + lax.optimization_barrier(jnp.sum(expert_sketch * expert_valid[None], axis=(1, 2, 3)))
    domains = prior_mix.shape[0]
    onehot = (domain_ids[:, None] == jnp.arange(domains, dtype=jnp.int32)[None, :]).astype(jnp.float32)
    domain_total = jnp.dot(score, onehot, precision=lax.Precision.HIGHEST)
    spread = jnp.sqrt(jnp.mean(domain_total * domain_total) + 1e-06)
    z_value = domain_total / spread
    mass = jnp.sum(prior_mix * jnp.exp(0.5 * z_value))
    return jnp.log(prior_mix) + 0.5 * z_value - jnp.log(mass)
```

```python
import functools

import jax
import jax.numpy as jnp
from jax import lax
from jax.experimental import pallas as pl
from jax.experimental.pallas import tpu as pltpu
from jax.sharding import PartitionSpec as P

MESH = pl.DeviceIdType.MESH
HIGHEST = lax.Precision.HIGHEST


def kernel(
    sizes,
    act, cot, pin, pout, eact, ecot, epin, epout, dval, evals, ids, prior,
    out,
    va, vc, vpin, vpout, vea, vec, vepin, vepout, vdv, vev, vids, vprior,
    dsend, drecv, esend, erecv, dg, eg, acc, rows,
    a_sem, c_sem, ea_sem, ec_sem, w_sem,
    ds_sem, dr_sem, es_sem, er_sem, row_send, row_recv,
):
    nd, ne, nt = sizes
    n = nd * ne * nt
    dp, ex, tx = lax.axis_index("dp"), lax.axis_index("expert"), lax.axis_index("tensor")
    me = (dp * ne + ex) * nt + tx
    layers, micro, q, rank = cot.shape[0], cot.shape[1], cot.shape[2], pin.shape[2]
    experts, qc = ecot.shape[1], ecot.shape[2]
    hidden = eact.shape[3]
    dim = ecot.shape[3]

    def split(k):
        return lax.div(k, micro), lax.rem(k, micro)

    def load_a(o, l, m):
        first = pl.multiple_of(lax.rem(tx + o, nt) * q, q)
        return pltpu.make_async_copy(act.at[l, m, pl.ds(first, q), :], va.at[o, l, m], a_sem.at[o, l, m])

    def load_ea(o, m):
        first = pl.multiple_of(lax.rem(tx + o, nt) * qc, qc)
        return pltpu.make_async_copy(eact.at[m, :, pl.ds(first, qc), :], vea.at[o, m], ea_sem.at[o, m])

    def load_c(l, m):
        return pltpu.make_async_copy(cot.at[l, m], vc.at[l, m], c_sem.at[l, m])

    def load_ec(m):
        return pltpu.make_async_copy(ecot.at[m], vec.at[m], ec_sem.at[m])

    weights = [
        pltpu.make_async_copy(src, dst, w_sem.at[i])
        for i, (src, dst) in enumerate(
            [(epin, vepin), (pin, vpin), (pout, vpout), (dval, vdv), (epout, vepout), (evals, vev), (ids, vids), (prior, vprior)]
        )
    ]
    w_epin, w_pin, w_pout, w_dval, w_epout, w_eval, w_ids, w_prior = weights

    def send_d(o, l, m):
        return pltpu.make_async_remote_copy(
            src_ref=dsend.at[o - 1, l, m], dst_ref=drecv.at[o - 1, l, m],
            send_sem=ds_sem.at[o - 1, l, m], recv_sem=dr_sem.at[o - 1, l, m],
            device_id={"dp": dp, "expert": ex, "tensor": lax.rem(tx + o, nt)}, device_id_type=MESH,
        )

    def send_e(o, m):
        return pltpu.make_async_remote_copy(
            src_ref=esend.at[o - 1, m], dst_ref=erecv.at[o - 1, m],
            send_sem=es_sem.at[o - 1, m], recv_sem=er_sem.at[o - 1, m],
            device_id={"dp": dp, "expert": ex, "tensor": lax.rem(tx + o, nt)}, device_id_type=MESH,
        )

    def peer(i):
        t = lax.rem(me + i, n)
        return {"dp": lax.div(t, ne * nt), "expert": lax.rem(lax.div(t, nt), ne), "tensor": lax.rem(t, nt)}

    barrier = pltpu.get_barrier_semaphore()

    @pl.loop(1, n)
    def _(i):
        pl.semaphore_signal(barrier, inc=1, device_id=peer(i), device_id_type=MESH)

    w_epin.start()
    for o in range(1, nt):
        load_ea(o, 0).start()
    for m in range(1, micro):
        for o in range(1, nt):
            load_ea(o, m).start()
    w_pin.start()

    acc[...] = jnp.zeros_like(acc)
    w_epin.wait()

    def expert_out(m):
        for o in range(1, nt):
            load_ea(o, m).wait()
            esend[o - 1, m] = jnp.dot(
                vea[o, m].reshape(experts * qc, hidden), vepin[...], preferred_element_type=jnp.float32
            )
        for l in range(layers):
            for o in range(1, nt):
                load_a(o, l, m).start()

    expert_out(0)
    pl.semaphore_wait(barrier, n - 1)
    for o in range(1, nt):
        send_e(o, 0).start()

    @pl.loop(1, micro)
    def _(m):
        expert_out(m)
        for o in range(1, nt):
            send_e(o, m).start()

    w_pout.start()
    w_dval.start()
    w_pin.wait()

    @pl.loop(0, layers * micro)
    def _(k):
        l, m = split(k)
        for o in range(1, nt):
            load_a(o, l, m).wait()
            dsend[o - 1, l, m] = jnp.dot(va[o, l, m], vpin[l], preferred_element_type=jnp.float32)
        load_a(0, l, m).start()
        load_c(l, m).start()
        for o in range(1, nt):
            send_d(o, l, m).start()

    w_epout.start()
    w_eval.start()
    for m in range(micro):
        load_ea(0, m).start()
        load_ec(m).start()
    w_ids.start()
    w_prior.start()
    w_pout.wait()
    w_dval.wait()

    def fold(m, value):
        acc[m] += jnp.sum(value.reshape(-1, 8, rank), axis=0)

    @pl.loop(0, layers * micro)
    def _(k):
        l, m = split(k)
        load_a(0, l, m).wait()
        load_c(l, m).wait()
        u = jnp.dot(va[0, l, m], vpin[l], preferred_element_type=jnp.float32)
        w = jnp.dot(vc[l, m], vpout[l], preferred_element_type=jnp.float32)
        g = lax.dot_general(
            w, vdv[l], (((1,), (1,)), ((), ())), precision=HIGHEST, preferred_element_type=jnp.float32
        )
        dg[l, m] = g
        fold(m, u * g)

    w_epout.wait()
    w_eval.wait()

    @pl.loop(0, micro)
    def _(m):
        load_ea(0, m).wait()
        load_ec(m).wait()
        u = jnp.dot(vea[0, m].reshape(experts * qc, hidden), vepin[...], preferred_element_type=jnp.float32)
        w = jnp.dot(vec[m].reshape(experts * qc, dim), vepout[...], preferred_element_type=jnp.float32)
        g = jnp.concatenate(
            [
                lax.dot_general(
                    w[e * qc : (e + 1) * qc], vev[e], (((1,), (1,)), ((), ())),
                    precision=HIGHEST, preferred_element_type=jnp.float32,
                )
                for e in range(experts)
            ],
            axis=0,
        )
        eg[m] = g
        fold(m, u * g)

    @pl.loop(0, micro)
    def _(m):
        for o in range(1, nt):
            send_e(o, m).wait()
            fold(m, erecv[o - 1, m] * eg[m])

    w_ids.wait()
    w_prior.wait()

    @pl.loop(0, layers * micro)
    def _(k):
        l, m = split(k)
        for o in range(1, nt):
            send_d(o, l, m).wait()
            fold(m, drecv[o - 1, l, m] * dg[l, m])

    lanes = rows.shape[2]
    lane = lax.broadcasted_iota(jnp.int32, (1, lanes), 1)
    part = jnp.zeros((1, lanes), jnp.float32)
    for m in range(micro):
        score = jnp.sum(jnp.sum(acc[m], axis=0, keepdims=True), axis=1, keepdims=True)
        part = part + jnp.where(lane == vids[m], score, 0.0)
    rows[me] = part

    def send_row(i):
        return pltpu.make_async_remote_copy(
            src_ref=rows.at[me], dst_ref=rows.at[me], send_sem=row_send, recv_sem=row_recv,
            device_id=peer(i), device_id_type=MESH,
        )

    @pl.loop(1, n)
    def _(i):
        send_row(i).start()

    others = rows.at[pl.ds(0, n - 1)]
    pltpu.make_async_copy(others, others, row_recv).wait()
    domains = prior.shape[1]
    total = jnp.sum(rows[...], axis=0)[:, :domains]
    spread = jnp.sqrt(jnp.sum(total * total, axis=1, keepdims=True) * (1.0 / domains) + 1e-06)
    z = total / spread
    mix = vprior[...]
    mass = jnp.sum(mix * jnp.exp(0.5 * z), axis=1, keepdims=True)
    out[...] = jnp.log(mix) + 0.5 * z - jnp.log(mass)
    pltpu.make_async_copy(others, others, row_send).wait()


def per_device(sizes, *args):
    (act, cot, pin, pout, eact, ecot, epin, epout, dval, evals, ids, prior) = args
    nd, ne, nt = sizes
    n = nd * ne * nt
    layers, micro, q, dim = cot.shape
    rank, feat = pin.shape[2], pin.shape[1]
    experts, qc, hidden = ecot.shape[1], ecot.shape[2], eact.shape[3]
    domains = prior.shape[0]
    lanes = -(-domains // 128) * 128
    bf, f32 = jnp.bfloat16, jnp.float32
    V, dma = pltpu.VMEM, pltpu.SemaphoreType.DMA
    logs = pl.pallas_call(
        functools.partial(kernel, sizes),
        out_shape=pltpu.VMEM((1, domains), f32),
        in_specs=[pl.BlockSpec(memory_space=pltpu.HBM)] * 12,
        out_specs=pl.BlockSpec(memory_space=pltpu.VMEM),
        scratch_shapes=[
            V((nt, layers, micro, q, feat), bf),
            V((layers, micro, q, dim), bf),
            V(pin.shape, bf),
            V(pout.shape, bf),
            V((nt, micro, experts, qc, hidden), bf),
            V((micro, experts, qc, dim), bf),
            V(epin.shape, bf),
            V(epout.shape, bf),
            V(dval.shape, f32),
            V(evals.shape, f32),
            pltpu.SMEM(ids.shape, jnp.int32),
            V((1, domains), f32),
            V((nt - 1, layers, micro, q, rank), f32),
            V((nt - 1, layers, micro, q, rank), f32),
            V((nt - 1, micro, experts * qc, rank), f32),
            V((nt - 1, micro, experts * qc, rank), f32),
            V((layers, micro, q, rank), f32),
            V((micro, experts * qc, rank), f32),
            V((micro, 8, rank), f32),
            V((n, 1, lanes), f32),
            dma((nt, layers, micro)),
            dma((layers, micro)),
            dma((nt, micro)),
            dma((micro,)),
            dma((8,)),
            dma((nt - 1, layers, micro)),
            dma((nt - 1, layers, micro)),
            dma((nt - 1, micro)),
            dma((nt - 1, micro)),
            dma,
            dma,
        ],
        compiler_params=pltpu.CompilerParams(
            collective_id=0, has_side_effects=True, vmem_limit_bytes=60 * 1024 * 1024
        ),
        name="align",
    )(act, cot, pin, pout, eact, ecot, epin, epout, dval, evals, ids, prior.reshape(1, domains))
    share = domains // nd
    return lax.dynamic_slice_in_dim(logs[0], lax.axis_index("dp") * share, share, 0)


def solution(mesh):
    sizes = (mesh.shape["dp"], mesh.shape["expert"], mesh.shape["tensor"])
    placed = (
        P(None, "dp", "expert", "tensor"),
        P(None, "dp", ("expert", "tensor"), None),
        P(None, "tensor", None),
        P(),
        P("dp", "expert", None, "tensor"),
        P("dp", "expert", "tensor", None),
        P("tensor", None),
        P(),
        P(),
        P("expert", None, None),
        P("dp"),
        P(),
    )
    return jax.shard_map(
        functools.partial(per_device, sizes), mesh=mesh, in_specs=placed, out_specs=P("dp"), check_vma=False
    )
```

```python
import functools

import jax
import jax.numpy as jnp
from jax import lax
from jax.experimental import pallas as pl
from jax.experimental.pallas import tpu as pltpu
from jax.sharding import PartitionSpec as P

MESH, LOGICAL = pl.DeviceIdType.MESH, pl.DeviceIdType.LOGICAL
HIGHEST = lax.Precision.HIGHEST
PIECES = 2
LENT = 3
ALONE = 4


def line_of(nd):
    stride = 2 if nd % 2 == 0 else 1
    return stride, nd // stride


def kernel(
    sizes,
    act, cot, pin, pout, eact, ecot, epin, epout, dval, evals, ids, prior,
    out,
    va, vc, vpin, vpout, vea, vec, vepin, vepout, vdv, vev, vids, vprior,
    dsend, drecv, esend, erecv, dg, eg, lu, lg, lmask, mask, acc, rows,
    a_sem, c_sem, ea_sem, w_sem, s_sem, e_sem, d_sem, lu_sem, lg_sem, lg_send, row_send, row_recv,
    line_sem, row_sem, tensor_sem,
):
    nd, ne, nt = sizes
    n = nd * ne * nt
    stride, places = line_of(nd)
    dp, ex, tx = lax.axis_index("dp"), lax.axis_index("expert"), lax.axis_index("tensor")
    me = (dp * ne + ex) * nt + tx
    place, row = lax.div(dp, stride), lax.rem(dp, stride)
    layers, micro, q, rank = cot.shape[0], cot.shape[1], cot.shape[2], pin.shape[2]
    experts, qc = ecot.shape[1], ecot.shape[2]
    hidden = eact.shape[3]
    dim = ecot.shape[3]
    h = q // PIECES
    blocks = layers * micro
    units = blocks * PIECES
    mate = (places - 1 - place) * stride + row

    def lends(at):
        return jnp.where(2 * at >= places, jnp.clip(2 * (at + row - (places + stride) // 2 + 1) - 1, 0, LENT), 0)

    lent, taken = lends(place), lends(places - 1 - place)

    def device(d=None, e=None, t=None):
        return {
            "dp": dp if d is None else d,
            "expert": ex if e is None else e,
            "tensor": tx if t is None else t,
        }

    def load_a(o, l):
        first = pl.multiple_of(lax.rem(tx + o, nt) * q, q)
        return pltpu.make_async_copy(act.at[l, :, pl.ds(first, q), :], va.at[o, l], a_sem.at[l])

    def load_ea(o, first_m, count, i):
        first = pl.multiple_of(lax.rem(tx + o, nt) * qc, qc)
        some = pl.ds(first_m, count)
        return pltpu.make_async_copy(eact.at[some, :, pl.ds(first, qc), :], vea.at[o, some], ea_sem.at[i])

    def load_c(l):
        return pltpu.make_async_copy(cot.at[l], vc.at[l], c_sem.at[l])

    load_ec = pltpu.make_async_copy(ecot, vec, ea_sem.at[1])

    def load_w(src, dst, i):
        return pltpu.make_async_copy(src, dst, w_sem.at[i])

    w_epin, w_pout, w_epout = load_w(epin, vepin, 0), load_w(pout, vpout, 0), load_w(epout, vepout, 0)
    w_pin, w_dval, w_eval = load_w(pin, vpin, 1), load_w(dval, vdv, 1), load_w(evals, vev, 1)
    w_ids, w_prior = load_w(ids, vids, 2), load_w(prior, vprior, 2)

    def rows_of(j, count=1):
        return pl.ds(pl.multiple_of(j * h, h), count * h)

    def opposite(o):
        return lax.rem(tx + o, nt)

    def send_d(o, j):
        i = jnp.minimum(j, LENT) + jnp.maximum(j - (units - ALONE - 1), 0)
        return pltpu.make_async_remote_copy(
            src_ref=dsend.at[o - 1, rows_of(j)], dst_ref=drecv.at[o - 1, rows_of(j)],
            send_sem=s_sem.at[0], recv_sem=d_sem.at[o - 1, i],
            device_id=device(t=opposite(o)), device_id_type=MESH,
        )

    def lend_u(o, j):
        return pltpu.make_async_remote_copy(
            src_ref=dsend.at[o - 1, rows_of(j)], dst_ref=lu.at[o - 1, rows_of(j)],
            send_sem=s_sem.at[0], recv_sem=lu_sem.at[o - 1, j],
            device_id=device(d=mate, t=opposite(o)), device_id_type=MESH,
        )

    def lend_g(j):
        return pltpu.make_async_remote_copy(
            src_ref=dg.at[rows_of(j)], dst_ref=lg.at[rows_of(j)],
            send_sem=lg_send.at[j], recv_sem=lg_sem.at[j],
            device_id=device(d=mate), device_id_type=MESH,
        )

    def lend_mask():
        return pltpu.make_async_remote_copy(
            src_ref=mask, dst_ref=lmask,
            send_sem=lg_send.at[LENT], recv_sem=lg_sem.at[LENT],
            device_id=device(d=mate), device_id_type=MESH,
        )

    def send_e(o, m, e0, count):
        part = pl.ds(e0 * qc, count * qc)
        return pltpu.make_async_remote_copy(
            src_ref=esend.at[o - 1, m, part], dst_ref=erecv.at[o - 1, m, part],
            send_sem=s_sem.at[1], recv_sem=e_sem,
            device_id=device(t=opposite(o)), device_id_type=MESH,
        )

    def landed(ref, sem):
        pltpu.make_async_copy(ref, ref, sem).wait()

    def signal(sem, who):
        pl.semaphore_signal(sem, inc=1, device_id=who, device_id_type=MESH)

    def tell_tensor(sem):
        for o in range(1, nt):
            signal(sem, device(t=opposite(o)))

    def tell_row(sem):
        for j in range(1, stride):
            signal(sem, device(d=place * stride + lax.rem(row + j, stride)))

    def tell_line(sem):
        @pl.when(place > 0)
        def _():
            signal(sem, device(d=dp - stride))

        @pl.when(place < places - 1)
        def _():
            signal(sem, device(d=dp + stride))

    on_line = (place > 0).astype(jnp.int32) + (place < places - 1).astype(jnp.int32)
    line_rounds = places - 1

    def hear_line(r):
        if r < line_rounds:
            pl.semaphore_wait(line_sem.at[r], on_line)

    def next_line(r):
        if r < line_rounds:
            tell_line(line_sem.at[r])

    w_epin.start()
    for o in range(1, nt):
        load_ea(o, 0, 1, 0).start()
    barrier = pltpu.get_barrier_semaphore()
    tell_tensor(barrier)
    for j in range(1, ne):
        signal(barrier, device(e=lax.rem(ex + j, ne)))
    tell_row(barrier)
    tell_line(barrier)
    for o in range(1, nt):
        load_ea(o, 1, micro - 1, 1).start()
    w_pin.start()
    w_ids.start()
    acc[...] = jnp.zeros_like(acc)

    def expert_out(o, m, e0, count):
        esend[o - 1, m, pl.ds(e0 * qc, count * qc)] = jnp.dot(
            vea[o, m, pl.ds(e0, count)].reshape(count * qc, hidden), vepin[...], preferred_element_type=jnp.float32
        )

    half = max(experts // 2, 1)
    w_epin.wait()
    for o in range(1, nt):
        load_ea(o, 0, 1, 0).wait()
        expert_out(o, 0, 0, half)
    pl.semaphore_wait(barrier, nt - 1 + ne - 1 + stride - 1 + on_line)
    for o in range(1, nt):
        send_e(o, 0, 0, half).start()
    for l in range(layers):
        for o in range(1, nt):
            load_a(o, l).start()
    w_pout.start()
    next_line(0)
    if half < experts:
        for o in range(1, nt):
            expert_out(o, 0, half, experts - half)
            send_e(o, 0, half, experts - half).start()
    for o in range(1, nt):
        load_ea(o, 1, micro - 1, 1).wait()

    @pl.loop(1, micro)
    def _(m):
        for o in range(1, nt):
            expert_out(o, m, 0, experts)
            send_e(o, m, 0, experts).start()

    w_pin.wait()
    w_dval.start()
    hear_line(0)
    next_line(1)
    for l in range(layers):
        for o in range(1, nt):
            load_a(o, l).wait()
        load_a(0, l).start()
        load_c(l).start()
        if l == layers - 1:
            hear_line(1)
            next_line(2)

        @pl.loop(0, micro)
        def _(m):
            k = l * micro + m
            for o in range(1, nt):
                dsend[o - 1, pl.ds(pl.multiple_of(k * q, q), q)] = jnp.dot(
                    va[o, l, m], vpin[l], preferred_element_type=jnp.float32
                )
                for p in range(PIECES):
                    j = k * PIECES + p

                    @pl.when(j >= lent)
                    def _():
                        send_d(o, j).start()

    load_ea(0, 0, micro, 0).start()
    load_ec.start()
    hear_line(2)
    for r in range(3, line_rounds):
        next_line(r)
        hear_line(r)
    tell_row(row_sem)
    w_pout.wait()
    w_dval.wait()
    w_epout.start()
    w_eval.start()
    w_ids.wait()
    w_prior.start()

    lanes = rows.shape[2]
    lane = lax.broadcasted_iota(jnp.int32, (1, lanes), 1)

    def domain_of(m):
        return jnp.where(lane == vids[m], 1.0, 0.0)

    for j in range(LENT):
        mask[j] = domain_of(j // PIECES % micro)

    @pl.when(lent > 0)
    def _():
        lend_mask().start()
        for j in range(LENT):

            @pl.when(j < lent)
            def _():
                for o in range(1, nt):
                    lend_u(o, j).start()

    def fold(m, value):
        acc[m] += jnp.sum(value.reshape(-1, 8, rank), axis=0)

    for l in range(layers):
        load_a(0, l).wait()
        load_c(l).wait()
        if l == layers - 1:
            pl.semaphore_wait(row_sem, stride - 1)
            tell_tensor(tensor_sem)

        @pl.loop(0, micro)
        def _(m):
            k = l * micro + m
            u = jnp.dot(va[0, l, m], vpin[l], preferred_element_type=jnp.float32)
            w = jnp.dot(vc[l, m], vpout[l], preferred_element_type=jnp.float32)
            g = lax.dot_general(
                w, vdv[l], (((1,), (1,)), ((), ())), precision=HIGHEST, preferred_element_type=jnp.float32
            )
            dg[pl.ds(pl.multiple_of(k * q, q), q)] = g
            fold(m, u * g)
            if l * micro * PIECES < LENT:
                for p in range(PIECES):

                    @pl.when(k * PIECES + p < lent)
                    def _():
                        lend_g(k * PIECES + p).start()

    w_epout.wait()
    w_eval.wait()
    load_ea(0, 0, micro, 0).wait()
    load_ec.wait()
    pl.semaphore_wait(tensor_sem, nt - 1)

    @pl.loop(0, micro)
    def _(m):
        u = jnp.dot(vea[0, m].reshape(experts * qc, hidden), vepin[...], preferred_element_type=jnp.float32)
        w = jnp.dot(vec[m].reshape(experts * qc, dim), vepout[...], preferred_element_type=jnp.float32)
        g = jnp.concatenate(
            [
                lax.dot_general(
                    w[e * qc : (e + 1) * qc], vev[e], (((1,), (1,)), ((), ())),
                    precision=HIGHEST, preferred_element_type=jnp.float32,
                )
                for e in range(experts)
            ],
            axis=0,
        )
        eg[m] = g
        fold(m, u * g)

    landed(erecv, e_sem)

    @pl.loop(0, micro)
    def _(m):
        for o in range(1, nt):
            fold(m, erecv[o - 1, m] * eg[m])

    w_prior.wait()

    def cross(o, j):
        return drecv[o - 1, rows_of(j)] * dg[rows_of(j)]

    def total_of(value):
        return jnp.sum(jnp.sum(value, axis=1, keepdims=True), axis=0, keepdims=True)

    for j in range(LENT):

        @pl.when(j >= lent)
        def _():
            for o in range(1, nt):
                landed(drecv.at[o - 1, rows_of(j)], d_sem.at[o - 1, j])
                fold(j // PIECES % micro, cross(o, j))

    rows[me] = jnp.zeros((1, lanes), jnp.float32)

    @pl.when(taken > 0)
    def _():
        landed(lmask, lg_sem.at[LENT])
        for j in range(LENT):

            @pl.when(j < taken)
            def _():
                landed(lg.at[rows_of(j)], lg_sem.at[j])
                value = jnp.zeros((8, rank), jnp.float32)
                for o in range(1, nt):
                    landed(lu.at[o - 1, rows_of(j)], lu_sem.at[o - 1, j])
                    both = lu[o - 1, rows_of(j)] * lg[rows_of(j)]
                    value = value + jnp.sum(both.reshape(-1, 8, rank), axis=0)
                rows[me] += lmask[j] * total_of(value)

    for o in range(1, nt):
        landed(drecv.at[o - 1, rows_of(LENT, units - ALONE - LENT)], d_sem.at[o - 1, LENT])

    @pl.loop(LENT, units - ALONE)
    def _(j):
        for o in range(1, nt):
            fold(lax.rem(lax.div(j, PIECES), micro), cross(o, j))

    last = [(o, j) for j in range(units - ALONE, units) for o in range(1, nt)]
    for o, j in last[:-1]:
        landed(drecv.at[o - 1, rows_of(j)], d_sem.at[o - 1, j - units + ALONE + LENT + 1])
        fold(j // PIECES % micro, cross(o, j))

    part = rows[me]
    for m in range(micro):
        part = part + domain_of(m) * total_of(acc[m])
    rows[me] = part
    chosen = domain_of(micro - 1)
    o, j = last[-1]
    landed(drecv.at[o - 1, rows_of(j)], d_sem.at[o - 1, ALONE + LENT])
    rows[me] += chosen * total_of(jnp.sum(cross(o, j).reshape(-1, 8, rank), axis=0))

    for i in range(1, n):
        t = me + i
        pltpu.make_async_remote_copy(
            src_ref=rows.at[me], dst_ref=rows.at[me], send_sem=row_send, recv_sem=row_recv,
            device_id=jnp.where(t < n, t, t - n), device_id_type=LOGICAL,
        ).start()

    for o in range(1, nt):
        landed(dsend.at[o - 1], s_sem.at[0])
    landed(esend, s_sem.at[1])

    @pl.when(lent > 0)
    def _():
        lend_mask().wait_send()
        for j in range(LENT):

            @pl.when(j < lent)
            def _():
                lend_g(j).wait_send()

    others = rows.at[pl.ds(0, n - 1)]
    landed(others, row_recv)
    domains = prior.shape[1]
    total = jnp.sum(rows[...], axis=0)[:, :domains]
    spread = jnp.sqrt(jnp.sum(total * total, axis=1, keepdims=True) * (1.0 / domains) + 1e-06)
    z = total / spread
    mix = vprior[...]
    mass = jnp.sum(mix * jnp.exp(0.5 * z), axis=1, keepdims=True)
    out[...] = jnp.log(mix) + 0.5 * z - jnp.log(mass)
    landed(others, row_send)


def per_device(sizes, *args):
    (act, cot, pin, pout, eact, ecot, epin, epout, dval, evals, ids, prior) = args
    nd, ne, nt = sizes
    n = nd * ne * nt
    places = line_of(nd)[1]
    layers, micro, q, dim = cot.shape
    rank, feat = pin.shape[2], pin.shape[1]
    experts, qc, hidden = ecot.shape[1], ecot.shape[2], eact.shape[3]
    domains = prior.shape[0]
    lanes = -(-domains // 128) * 128
    lent = LENT * (q // PIECES)
    bf, f32 = jnp.bfloat16, jnp.float32
    V, dma, regular = pltpu.VMEM, pltpu.SemaphoreType.DMA, pltpu.SemaphoreType.REGULAR
    logs = pl.pallas_call(
        functools.partial(kernel, sizes),
        out_shape=pltpu.VMEM((1, domains), f32),
        in_specs=[pl.BlockSpec(memory_space=pltpu.HBM)] * 12,
        out_specs=pl.BlockSpec(memory_space=pltpu.VMEM),
        scratch_shapes=[
            V((nt, layers, micro, q, feat), bf),
            V((layers, micro, q, dim), bf),
            V(pin.shape, bf),
            V(pout.shape, bf),
            V((nt, micro, experts, qc, hidden), bf),
            V((micro, experts, qc, dim), bf),
            V(epin.shape, bf),
            V(epout.shape, bf),
            V(dval.shape, f32),
            V(evals.shape, f32),
            pltpu.SMEM(ids.shape, jnp.int32),
            V((1, domains), f32),
            V((nt - 1, layers * micro * q, rank), f32),
            V((nt - 1, layers * micro * q, rank), f32),
            V((nt - 1, micro, experts * qc, rank), f32),
            V((nt - 1, micro, experts * qc, rank), f32),
            V((layers * micro * q, rank), f32),
            V((micro, experts * qc, rank), f32),
            V((nt - 1, lent, rank), f32),
            V((lent, rank), f32),
            V((LENT, 1, lanes), f32),
            V((LENT, 1, lanes), f32),
            V((micro, 8, rank), f32),
            V((n, 1, lanes), f32),
            dma((layers,)),
            dma((layers,)),
            dma((2,)),
            dma((3,)),
            dma((2,)),
            dma,
            dma((nt - 1, LENT + 1 + ALONE)),
            dma((nt - 1, LENT)),
            dma((LENT + 1,)),
            dma((LENT + 1,)),
            dma,
            dma,
            regular((max(places - 1, 1),)),
            regular,
            regular,
        ],
        compiler_params=pltpu.CompilerParams(
            collective_id=0, has_side_effects=True, vmem_limit_bytes=60 * 1024 * 1024
        ),
        name="align",
    )(act, cot, pin, pout, eact, ecot, epin, epout, dval, evals, ids, prior.reshape(1, domains))
    share = domains // nd
    return lax.dynamic_slice_in_dim(logs[0], lax.axis_index("dp") * share, share, 0)


def solution(mesh):
    sizes = (mesh.shape["dp"], mesh.shape["expert"], mesh.shape["tensor"])
    placed = (
        P(None, "dp", "expert", "tensor"),
        P(None, "dp", ("expert", "tensor"), None),
        P(None, "tensor", None),
        P(),
        P("dp", "expert", None, "tensor"),
        P("dp", "expert", "tensor", None),
        P("tensor", None),
        P(),
        P(),
        P("expert", None, None),
        P("dp"),
        P(),
    )
    return jax.shard_map(
        functools.partial(per_device, sizes), mesh=mesh, in_specs=placed, out_specs=P("dp"), check_vma=False
    )
```

```python
import functools

import jax
import jax.numpy as jnp
from jax import lax
from jax.experimental import pallas as pl
from jax.experimental.pallas import tpu as pltpu
from jax.sharding import PartitionSpec as P

MESH, LOGICAL = pl.DeviceIdType.MESH, pl.DeviceIdType.LOGICAL
HIGHEST = lax.Precision.HIGHEST
BATCH = 2
PIECES = 2
LENT = 3
GIVEN = 2
ACROSS = LENT + GIVEN
CROWD = ACROSS + 1
ALONE = 3


def line_of(nd):
    stride = 2 if nd % 2 == 0 else 1
    return stride, nd // stride


def kernel(
    sizes,
    act, cot, pin, pout, eact, ecot, epin, epout, dval, evals, ids, prior,
    out,
    va, vc, vpin, vpout, vea, vec, vepin, vepout, vdv, vev, vids, vprior,
    dsend, drecv, esend, erecv, dg, eg, lu, lg, lmask, mask, ru, hu, hg, yru, yhu, yhg, ymask, acc, fin, rows,
    a_sem, c_sem, ea_sem, w_sem, s_sem, e_sem, d_sem, l_sem, lg_send, r_sem, hu_sem, r_send, y_sem, y_send, row_send, row_recv,
    line_sem, row_sem, tensor_sem,
):
    nd, ne, nt = sizes
    n = nd * ne * nt
    stride, places = line_of(nd)
    dp, ex, tx = lax.axis_index("dp"), lax.axis_index("expert"), lax.axis_index("tensor")
    me = (dp * ne + ex) * nt + tx
    place, row = lax.div(dp, stride), lax.rem(dp, stride)
    layers, micro, q, rank = cot.shape[0], cot.shape[1], cot.shape[2], pin.shape[2]
    experts, qc = ecot.shape[1], ecot.shape[2]
    hidden = eact.shape[3]
    dim = ecot.shape[3]
    h = q // PIECES
    blocks = layers * micro
    units = blocks * PIECES
    batch = BATCH if micro % BATCH == 0 else 1
    mate = (places - 1 - place) * stride + row

    def lends(at):
        return jnp.where(2 * at >= places, jnp.clip(2 * (at + row - (places + stride) // 2 + 1) - row, 0, LENT), 0)

    lent, taken = lends(place), lends(places - 1 - place)
    near = 2 * place < places
    over, guest = ((row == 1) & near, (row == 0) & near) if stride > 1 else (row < 0, row < 0)
    giver, helper = (ex == 0, ex == 1) if ne > 1 else (ex < 0, ex < 0)

    def device(d=None, e=None, t=None):
        return {
            "dp": dp if d is None else d,
            "expert": ex if e is None else e,
            "tensor": tx if t is None else t,
        }

    def load_a(o, l):
        first = pl.multiple_of(lax.rem(tx + o, nt) * q, q)
        return pltpu.make_async_copy(act.at[l, :, pl.ds(first, q), :], va.at[o, l], a_sem.at[l])

    def load_ea(o, first_m, count, i):
        first = pl.multiple_of(lax.rem(tx + o, nt) * qc, qc)
        some = pl.ds(first_m, count)
        return pltpu.make_async_copy(eact.at[some, :, pl.ds(first, qc), :], vea.at[o, some], ea_sem.at[i])

    def load_c(l):
        return pltpu.make_async_copy(cot.at[l], vc.at[l], c_sem.at[l])

    load_ec = pltpu.make_async_copy(ecot, vec, ea_sem.at[1])

    def load_w(src, dst, i):
        return pltpu.make_async_copy(src, dst, w_sem.at[i])

    w_epin, w_pout, w_epout = load_w(epin, vepin, 0), load_w(pout, vpout, 0), load_w(epout, vepout, 0)
    w_pin, w_dval, w_eval = load_w(pin, vpin, 1), load_w(dval, vdv, 1), load_w(evals, vev, 1)
    w_ids, w_prior = load_w(ids, vids, 2), load_w(prior, vprior, 2)

    def rows_of(j, count=1):
        return pl.ds(pl.multiple_of(j * h, h), count * h)

    def opposite(o):
        return lax.rem(tx + o, nt)

    def send_d(o, j):
        i = jnp.maximum(j - (units - ALONE - 1), 0)
        for first in (LENT, ACROSS, CROWD):
            i = i + jnp.where(j >= first, 1, 0)
        return pltpu.make_async_remote_copy(
            src_ref=dsend.at[o - 1, rows_of(j)], dst_ref=drecv.at[o - 1, rows_of(j)],
            send_sem=s_sem.at[0], recv_sem=d_sem.at[o - 1, i],
            device_id=device(t=opposite(o)), device_id_type=MESH,
        )

    def lend_u(o, j):
        return pltpu.make_async_remote_copy(
            src_ref=dsend.at[o - 1, rows_of(j)], dst_ref=lu.at[o - 1, rows_of(j)],
            send_sem=s_sem.at[0], recv_sem=l_sem.at[1 + o],
            device_id=device(d=mate, t=opposite(o)), device_id_type=MESH,
        )

    def lend_g(j):
        return pltpu.make_async_remote_copy(
            src_ref=dg.at[rows_of(j)], dst_ref=lg.at[rows_of(j)],
            send_sem=lg_send.at[0], recv_sem=l_sem.at[0],
            device_id=device(d=mate), device_id_type=MESH,
        )

    def lend_mask():
        return pltpu.make_async_remote_copy(
            src_ref=mask.at[pl.ds(0, LENT)], dst_ref=lmask,
            send_sem=lg_send.at[1], recv_sem=l_sem.at[1],
            device_id=device(d=mate), device_id_type=MESH,
        )

    given = rows_of(LENT, GIVEN)

    def give_u(o):
        return pltpu.make_async_remote_copy(
            src_ref=dsend.at[o - 1, given], dst_ref=ru.at[o - 1],
            send_sem=s_sem.at[0], recv_sem=r_sem.at[o],
            device_id=device(e=1), device_id_type=MESH,
        )

    def give_g():
        return pltpu.make_async_remote_copy(
            src_ref=dg.at[given], dst_ref=hg,
            send_sem=lg_send.at[2], recv_sem=r_sem.at[0],
            device_id=device(e=1), device_id_type=MESH,
        )

    def pass_on(o, i):
        return pltpu.make_async_remote_copy(
            src_ref=ru.at[o - 1, rows_of(i)], dst_ref=hu.at[o - 1, rows_of(i)],
            send_sem=r_send, recv_sem=hu_sem.at[o - 1, i],
            device_id=device(t=opposite(o)), device_id_type=MESH,
        )

    def pass_over_u(o):
        return pltpu.make_async_remote_copy(
            src_ref=dsend.at[o - 1, rows_of(ACROSS)], dst_ref=yru.at[o - 1],
            send_sem=s_sem.at[0], recv_sem=y_sem.at[1 + o],
            device_id=device(d=place * stride), device_id_type=MESH,
        )

    def pass_over_g():
        return pltpu.make_async_remote_copy(
            src_ref=dg.at[rows_of(ACROSS)], dst_ref=yhg, send_sem=y_send.at[0], recv_sem=y_sem.at[0],
            device_id=device(d=place * stride), device_id_type=MESH,
        )

    def pass_over_mask():
        return pltpu.make_async_remote_copy(
            src_ref=mask.at[LENT], dst_ref=ymask, send_sem=y_send.at[1], recv_sem=y_sem.at[1],
            device_id=device(d=place * stride), device_id_type=MESH,
        )

    def pass_through(o):
        return pltpu.make_async_remote_copy(
            src_ref=yru.at[o - 1], dst_ref=yhu.at[o - 1],
            send_sem=y_send.at[1 + o], recv_sem=y_sem.at[nt + o],
            device_id=device(t=opposite(o)), device_id_type=MESH,
        )

    def send_e(o, m, e0, count):
        part = pl.ds(e0 * qc, count * qc)
        return pltpu.make_async_remote_copy(
            src_ref=esend.at[o - 1, m, part], dst_ref=erecv.at[o - 1, m, part],
            send_sem=s_sem.at[1], recv_sem=e_sem,
            device_id=device(t=opposite(o)), device_id_type=MESH,
        )

    def landed(ref, sem):
        pltpu.make_async_copy(ref, ref, sem).wait()

    def signal(sem, who):
        pl.semaphore_signal(sem, inc=1, device_id=who, device_id_type=MESH)

    def tell_tensor(sem):
        for o in range(1, nt):
            signal(sem, device(t=opposite(o)))

    def tell_row(sem):
        for j in range(1, stride):
            signal(sem, device(d=place * stride + lax.rem(row + j, stride)))

    def tell_line(sem):
        @pl.when(place > 0)
        def _():
            signal(sem, device(d=dp - stride))

        @pl.when(place < places - 1)
        def _():
            signal(sem, device(d=dp + stride))

    on_line = (place > 0).astype(jnp.int32) + (place < places - 1).astype(jnp.int32)
    line_rounds = places - 1

    def hear_line(r):
        if r < line_rounds:
            pl.semaphore_wait(line_sem.at[r], on_line)

    def next_line(r):
        if r < line_rounds:
            tell_line(line_sem.at[r])

    w_epin.start()
    for o in range(1, nt):
        load_ea(o, 0, 1, 0).start()
    barrier = pltpu.get_barrier_semaphore()
    tell_tensor(barrier)
    for j in range(1, ne):
        signal(barrier, device(e=lax.rem(ex + j, ne)))
    tell_row(barrier)
    tell_line(barrier)
    for o in range(1, nt):
        load_ea(o, 1, micro - 1, 1).start()
    w_pin.start()
    w_ids.start()
    acc[...] = jnp.zeros_like(acc)

    def expert_out(o, m, e0, count):
        esend[o - 1, m, pl.ds(e0 * qc, count * qc)] = jnp.dot(
            vea[o, m, pl.ds(e0, count)].reshape(count * qc, hidden), vepin[...], preferred_element_type=jnp.float32
        )

    half = max(experts // 2, 1)
    w_epin.wait()
    for o in range(1, nt):
        load_ea(o, 0, 1, 0).wait()
        expert_out(o, 0, 0, half)
    pl.semaphore_wait(barrier, nt - 1 + ne - 1 + stride - 1 + on_line)
    for o in range(1, nt):
        send_e(o, 0, 0, half).start()
    for l in range(layers):
        for o in range(1, nt):
            load_a(o, l).start()
    w_pout.start()
    next_line(0)
    if half < experts:
        for o in range(1, nt):
            expert_out(o, 0, half, experts - half)
            send_e(o, 0, half, experts - half).start()
    for o in range(1, nt):
        load_ea(o, 1, micro - 1, 1).wait()

    @pl.loop(1, micro)
    def _(m):
        for o in range(1, nt):
            expert_out(o, m, 0, experts)
            send_e(o, m, 0, experts).start()

    w_pin.wait()
    w_dval.start()
    hear_line(0)
    next_line(1)
    for l in range(layers):
        for o in range(1, nt):
            load_a(o, l).wait()
        load_a(0, l).start()
        load_c(l).start()
        if l == layers - 1:
            hear_line(1)
            next_line(2)

        for first in range(0, micro, batch):
            for o in range(1, nt):
                dsend[o - 1, pl.ds((l * micro + first) * q, batch * q)] = jnp.dot(
                    va[o, l, first : first + batch].reshape(batch * q, pin.shape[1]), vpin[l],
                    preferred_element_type=jnp.float32,
                )

            @pl.loop(0, batch * PIECES)
            def _(i):
                j = (l * micro + first) * PIECES + i
                for o in range(1, nt):
                    kept = (giver & (j >= LENT) & (j < ACROSS)) | (over & (j == ACROSS))

                    @pl.when((j >= lent) & ~kept)
                    def _():
                        send_d(o, j).start()

                    @pl.when(giver & (j == ACROSS - 1))
                    def _():
                        give_u(o).start()

    load_ea(0, 0, micro, 0).start()
    load_ec.start()

    @pl.when(helper)
    def _():
        for o in range(1, nt):
            landed(ru.at[o - 1], r_sem.at[o])
            for i in range(GIVEN):
                pass_on(o, i).start()

    hear_line(2)
    for r in range(3, line_rounds):
        next_line(r)
        hear_line(r)
    tell_row(row_sem)
    w_pout.wait()
    w_dval.wait()
    w_epout.start()
    w_eval.start()
    w_ids.wait()
    w_prior.start()

    lanes = rows.shape[2]
    lane = lax.broadcasted_iota(jnp.int32, (1, lanes), 1)

    def domain_of(m):
        return jnp.where(lane == vids[m], 1.0, 0.0)

    for j in range(LENT):
        mask[j] = domain_of(j // PIECES % micro)
    mask[LENT] = domain_of(ACROSS // PIECES % micro)

    @pl.when(lent > 0)
    def _():
        lend_mask().start()
        for j in range(LENT):

            @pl.when(j < lent)
            def _():
                for o in range(1, nt):
                    lend_u(o, j).start()

    @pl.when(over)
    def _():
        pass_over_mask().start()
        for o in range(1, nt):
            pass_over_u(o).start()

    def fold(m, value):
        acc[m] += jnp.sum(value.reshape(-1, 8, rank), axis=0)

    def folds(some, value):
        acc[some] += jnp.sum(value.reshape(batch, -1, 8, rank), axis=1)

    for l in range(layers):
        load_a(0, l).wait()
        load_c(l).wait()
        if l == layers - 1:
            pl.semaphore_wait(row_sem, stride - 1)
            tell_tensor(tensor_sem)

        for first in range(0, micro, batch):
            some = slice(first, first + batch)
            u = jnp.dot(
                va[0, l, some].reshape(batch * q, pin.shape[1]), vpin[l], preferred_element_type=jnp.float32
            )
            w = jnp.dot(vc[l, some].reshape(batch * q, dim), vpout[l], preferred_element_type=jnp.float32)
            g = lax.dot_general(
                w, vdv[l], (((1,), (1,)), ((), ())), precision=HIGHEST, preferred_element_type=jnp.float32
            )
            dg[pl.ds((l * micro + first) * q, batch * q)] = g
            folds(some, u * g)
            done = range((l * micro + first) * PIECES, (l * micro + first + batch) * PIECES)
            for j in range(LENT):
                if j in done:

                    @pl.when(j < lent)
                    def _():
                        lend_g(j).start()

            if ACROSS - 1 in done:

                @pl.when(giver)
                def _():
                    give_g().start()

            if ACROSS in done:

                @pl.when(over)
                def _():
                    pass_over_g().start()

    w_epout.wait()
    w_eval.wait()
    load_ea(0, 0, micro, 0).wait()
    load_ec.wait()
    pl.semaphore_wait(tensor_sem, nt - 1)

    for first in range(0, micro, batch):
        some = slice(first, first + batch)
        u = jnp.dot(
            vea[0, some].reshape(batch * experts * qc, hidden), vepin[...], preferred_element_type=jnp.float32
        )
        w = jnp.dot(vec[some].reshape(batch * experts * qc, dim), vepout[...], preferred_element_type=jnp.float32)
        w = w.reshape(batch, experts, qc, rank)
        g = [
            lax.dot_general(
                w[:, e].reshape(batch * qc, rank), vev[e], (((1,), (1,)), ((), ())),
                precision=HIGHEST, preferred_element_type=jnp.float32,
            ).reshape(batch, 1, qc, rank)
            for e in range(experts)
        ]
        g = jnp.concatenate(g, axis=1).reshape(batch, experts * qc, rank)
        eg[some] = g
        folds(some, u.reshape(batch, experts * qc, rank) * g)
        if first == 0:

            @pl.when(guest)
            def _():
                for o in range(1, nt):
                    landed(yru.at[o - 1], y_sem.at[1 + o])
                    pass_through(o).start()

    landed(erecv, e_sem)

    @pl.loop(0, micro)
    def _(m):
        for o in range(1, nt):
            fold(m, erecv[o - 1, m] * eg[m])

    w_prior.wait()

    def cross(o, j):
        return drecv[o - 1, rows_of(j)] * dg[rows_of(j)]

    def total_of(value):
        return jnp.sum(jnp.sum(value, axis=1, keepdims=True), axis=0, keepdims=True)

    for c in range(LENT):

        @pl.when(lent == c)
        def _():
            for o in range(1, nt):
                landed(drecv.at[o - 1, rows_of(c, LENT - c)], d_sem.at[o - 1, 0])
                for j in range(c, LENT):
                    fold(j // PIECES % micro, cross(o, j))

    rows[me] = jnp.zeros((1, lanes), jnp.float32)

    @pl.when(taken > 0)
    def _():
        landed(lmask, l_sem.at[1])
        for c in range(1, LENT + 1):

            @pl.when(taken == c)
            def _():
                landed(lg.at[rows_of(0, c)], l_sem.at[0])
                for o in range(1, nt):
                    landed(lu.at[o - 1, rows_of(0, c)], l_sem.at[1 + o])

        for j in range(LENT):

            @pl.when(j < taken)
            def _():
                value = jnp.zeros((8, rank), jnp.float32)
                for o in range(1, nt):
                    both = lu[o - 1, rows_of(j)] * lg[rows_of(j)]
                    value = value + jnp.sum(both.reshape(-1, 8, rank), axis=0)
                rows[me] += lmask[j] * total_of(value)

    @pl.when(~giver)
    def _():
        for o in range(1, nt):
            landed(drecv.at[o - 1, given], d_sem.at[o - 1, 1])
            for j in range(LENT, ACROSS):
                fold(j // PIECES % micro, cross(o, j))

    @pl.when(~over)
    def _():
        for o in range(1, nt):
            landed(drecv.at[o - 1, rows_of(ACROSS)], d_sem.at[o - 1, 2])
            fold(ACROSS // PIECES % micro, cross(o, ACROSS))

    for o in range(1, nt):
        landed(drecv.at[o - 1, rows_of(CROWD, units - ALONE - CROWD)], d_sem.at[o - 1, 3])

    @pl.loop(CROWD, units - ALONE)
    def _(j):
        for o in range(1, nt):
            fold(lax.rem(lax.div(j, PIECES), micro), cross(o, j))

    def take(o, j):
        landed(drecv.at[o - 1, rows_of(j)], d_sem.at[o - 1, j - units + ALONE + 4])

    def take_given(o, i):
        landed(hu.at[o - 1, rows_of(i)], hu_sem.at[o - 1, i])
        return hu[o - 1, rows_of(i)] * hg[rows_of(i)]

    def shorter(value):
        return jnp.sum(value.reshape(-1, 8, rank), axis=0)

    last = [(o, j) for j in range(units - ALONE, units) for o in range(1, nt)]
    for o, j in last[:-1]:
        take(o, j)
        fold(j // PIECES % micro, cross(o, j))
    o, j = last[-1]

    @pl.when(guest)
    def _():
        landed(ymask, y_sem.at[1])
        landed(yhg, y_sem.at[0])
        value = jnp.zeros((8, rank), jnp.float32)
        for o_ in range(1, nt):
            landed(yhu.at[o_ - 1], y_sem.at[nt + o_])
            value = value + shorter(yhu[o_ - 1] * yhg[...])
        rows[me] += ymask[...] * total_of(value)

    @pl.when(helper)
    def _():
        take(o, j)
        fold(micro - 1, cross(o, j))
        landed(hg, r_sem.at[0])
        for i in range(GIVEN):
            for o_ in range(1, nt):
                if (i, o_) != (GIVEN - 1, nt - 1):
                    fold((LENT + i) // PIECES % micro, take_given(o_, i))

    part = rows[me]
    for m in range(micro):
        part = part + domain_of(m) * total_of(acc[m])
    rows[me] = part
    chosen = jnp.where(helper, domain_of((ACROSS - 1) // PIECES % micro), domain_of(micro - 1))

    @pl.when(helper)
    def _():
        fin[...] = shorter(take_given(nt - 1, GIVEN - 1))

    @pl.when(~helper)
    def _():
        take(o, j)
        fin[...] = shorter(cross(o, j))

    rows[me] += chosen * total_of(fin[...])

    for i in range(n - 1):
        pltpu.make_async_remote_copy(
            src_ref=rows.at[me], dst_ref=rows.at[me], send_sem=row_send, recv_sem=row_recv,
            device_id=i + (me <= i).astype(jnp.int32), device_id_type=LOGICAL,
        ).start()

    for o in range(1, nt):
        landed(dsend.at[o - 1], s_sem.at[0])
    landed(esend, s_sem.at[1])

    @pl.when(lent > 0)
    def _():
        lend_mask().wait_send()
        for c in range(1, LENT + 1):

            @pl.when(lent == c)
            def _():
                landed(dg.at[rows_of(0, c)], lg_send.at[0])

    @pl.when(giver)
    def _():
        give_g().wait_send()

    @pl.when(helper)
    def _():
        landed(ru, r_send)
    @pl.when(over)
    def _():
        pass_over_mask().wait_send()
        pass_over_g().wait_send()

    @pl.when(guest)
    def _():
        for o in range(1, nt):
            pass_through(o).wait_send()

    others = rows.at[pl.ds(0, n - 1)]
    landed(others, row_recv)
    domains = prior.shape[1]
    total = jnp.sum(rows[...], axis=0)[:, :domains]
    spread = jnp.sqrt(jnp.sum(total * total, axis=1, keepdims=True) * (1.0 / domains) + 1e-06)
    z = total / spread
    mix = vprior[...]
    mass = jnp.sum(mix * jnp.exp(0.5 * z), axis=1, keepdims=True)
    out[...] = jnp.log(mix) + 0.5 * z - jnp.log(mass)
    landed(others, row_send)


def per_device(sizes, *args):
    (act, cot, pin, pout, eact, ecot, epin, epout, dval, evals, ids, prior) = args
    nd, ne, nt = sizes
    n = nd * ne * nt
    places = line_of(nd)[1]
    layers, micro, q, dim = cot.shape
    rank, feat = pin.shape[2], pin.shape[1]
    experts, qc, hidden = ecot.shape[1], ecot.shape[2], eact.shape[3]
    domains = prior.shape[0]
    lanes = -(-domains // 128) * 128
    lent, given = LENT * (q // PIECES), GIVEN * (q // PIECES)
    bf, f32 = jnp.bfloat16, jnp.float32
    V, dma, regular = pltpu.VMEM, pltpu.SemaphoreType.DMA, pltpu.SemaphoreType.REGULAR
    logs = pl.pallas_call(
        functools.partial(kernel, sizes),
        out_shape=pltpu.VMEM((1, domains), f32),
        in_specs=[pl.BlockSpec(memory_space=pltpu.HBM)] * 12,
        out_specs=pl.BlockSpec(memory_space=pltpu.VMEM),
        scratch_shapes=[
            V((nt, layers, micro, q, feat), bf),
            V((layers, micro, q, dim), bf),
            V(pin.shape, bf),
            V(pout.shape, bf),
            V((nt, micro, experts, qc, hidden), bf),
            V((micro, experts, qc, dim), bf),
            V(epin.shape, bf),
            V(epout.shape, bf),
            V(dval.shape, f32),
            V(evals.shape, f32),
            pltpu.SMEM(ids.shape, jnp.int32),
            V((1, domains), f32),
            V((nt - 1, layers * micro * q, rank), f32),
            V((nt - 1, layers * micro * q, rank), f32),
            V((nt - 1, micro, experts * qc, rank), f32),
            V((nt - 1, micro, experts * qc, rank), f32),
            V((layers * micro * q, rank), f32),
            V((micro, experts * qc, rank), f32),
            V((nt - 1, lent, rank), f32),
            V((lent, rank), f32),
            V((LENT, 1, lanes), f32),
            V((LENT + 1, 1, lanes), f32),
            V((nt - 1, given, rank), f32),
            V((nt - 1, given, rank), f32),
            V((given, rank), f32),
            V((nt - 1, q // PIECES, rank), f32),
            V((nt - 1, q // PIECES, rank), f32),
            V((q // PIECES, rank), f32),
            V((1, lanes), f32),
            V((micro, 8, rank), f32),
            V((8, rank), f32),
            V((n, 1, lanes), f32),
            dma((layers,)),
            dma((layers,)),
            dma((2,)),
            dma((3,)),
            dma((2,)),
            dma,
            dma((nt - 1, 4 + ALONE)),
            dma((1 + nt,)),
            dma((3,)),
            dma((nt,)),
            dma((nt - 1, GIVEN)),
            dma,
            dma((2 * nt,)),
            dma((1 + nt,)),
            dma,
            dma,
            regular((max(places - 1, 1),)),
            regular,
            regular,
        ],
        compiler_params=pltpu.CompilerParams(
            collective_id=0, has_side_effects=True, vmem_limit_bytes=60 * 1024 * 1024
        ),
        name="align",
    )(act, cot, pin, pout, eact, ecot, epin, epout, dval, evals, ids, prior.reshape(1, domains))
    share = domains // nd
    return lax.dynamic_slice_in_dim(logs[0], lax.axis_index("dp") * share, share, 0)


def solution(mesh):
    sizes = (mesh.shape["dp"], mesh.shape["expert"], mesh.shape["tensor"])
    placed = (
        P(None, "dp", "expert", "tensor"),
        P(None, "dp", ("expert", "tensor"), None),
        P(None, "tensor", None),
        P(),
        P("dp", "expert", None, "tensor"),
        P("dp", "expert", "tensor", None),
        P("tensor", None),
        P(),
        P(),
        P("expert", None, None),
        P("dp"),
        P(),
    )
    return jax.shard_map(
        functools.partial(per_device, sizes), mesh=mesh, in_specs=placed, out_specs=P("dp"), check_vma=False
    )
```

```python
import functools

import jax
import jax.numpy as jnp
from jax import lax
from jax.experimental import pallas as pl
from jax.experimental.pallas import tpu as pltpu
from jax.sharding import PartitionSpec as P

MESH, LOGICAL = pl.DeviceIdType.MESH, pl.DeviceIdType.LOGICAL
HIGHEST = lax.Precision.HIGHEST
BATCH = 2
PIECES = 4
LENT = 5
GIVEN = 6
OVER = 2
FIRST = LENT + GIVEN
CROWD = FIRST + OVER
ALONE = 2


def line_of(nd):
    stride = 2 if nd % 2 == 0 else 1
    return stride, nd // stride


def kernel(
    sizes,
    act, cot, pin, pout, eact, ecot, epin, epout, dval, evals, ids, prior,
    out,
    va, vc, vpin, vpout, vea, vec, vepin, vepout, vdv, vev, vids, vprior,
    dsend, drecv, esend, erecv, dg, eg, lu, lg, lmask, mask, ru, hu, hg, yru, yhu, yhg, acc, fin, rows,
    a_sem, ea_sem, w_sem, s_sem, e_sem, d_sem, l_sem, u_send, r_sem, hu_sem, y_sem, row_send, row_recv,
    line_sem, row_sem, tensor_sem,
):
    nd, ne, nt = sizes
    n = nd * ne * nt
    stride, places = line_of(nd)
    dp, ex, tx = lax.axis_index("dp"), lax.axis_index("expert"), lax.axis_index("tensor")
    me = (dp * ne + ex) * nt + tx
    place, row = lax.div(dp, stride), lax.rem(dp, stride)
    layers, micro, q, rank = cot.shape[0], cot.shape[1], cot.shape[2], pin.shape[2]
    experts, qc = ecot.shape[1], ecot.shape[2]
    hidden = eact.shape[3]
    dim = ecot.shape[3]
    h = q // PIECES
    blocks = layers * micro
    units = blocks * PIECES
    batch = BATCH if micro % BATCH == 0 else 1
    mate = (places - 1 - place) * stride + row

    def lends(at):
        return jnp.where(2 * at >= places, jnp.clip(3 * (at + row - (places + stride) // 2 + 1) - row, 0, LENT), 0)

    lent, taken = lends(place), lends(places - 1 - place)
    near = 2 * place < places
    over, guest = ((row == 1) & near, (row == 0) & near) if stride > 1 else (row < 0, row < 0)
    giver, helper = (ex == 0, ex == 1) if ne > 1 else (ex < 0, ex < 0)

    def kept(j):
        return (j < lent) | (giver & (j >= LENT) & (j < FIRST)) | (over & (j >= FIRST) & (j < CROWD))

    def count_of(flag):
        return jnp.where(flag, 1, 0)

    def device(d=None, e=None, t=None):
        return {
            "dp": dp if d is None else d,
            "expert": ex if e is None else e,
            "tensor": tx if t is None else t,
        }

    def load_a(o, l):
        first = pl.multiple_of(lax.rem(tx + o, nt) * q, q)
        return pltpu.make_async_copy(act.at[l, :, pl.ds(first, q), :], va.at[o * layers + l], a_sem.at[l])

    def load_ea(o, first_m, count, i):
        first = pl.multiple_of(lax.rem(tx + o, nt) * qc, qc)
        some = pl.ds(first_m, count)
        return pltpu.make_async_copy(eact.at[some, :, pl.ds(first, qc), :], vea.at[o, some], ea_sem.at[i])

    def load_c(l):
        return pltpu.make_async_copy(cot.at[l], vc.at[l], a_sem.at[l])

    load_ec = pltpu.make_async_copy(ecot, vec, ea_sem.at[1])

    def load_w(src, dst, i):
        return pltpu.make_async_copy(src, dst, w_sem.at[i])

    w_epin, w_pout, w_epout = load_w(epin, vepin, 0), load_w(pout, vpout, 0), load_w(epout, vepout, 0)
    w_pin, w_dval, w_eval = load_w(pin, vpin, 1), load_w(dval, vdv, 1), load_w(evals, vev, 1)
    w_ids, w_prior = pltpu.make_async_copy(ids, vids, ea_sem.at[0]), load_w(prior, vprior, 0)

    def rows_of(j, count=1):
        return pl.ds(pl.multiple_of(j * h, h), count * h)

    def opposite(o):
        return lax.rem(tx + o, nt)

    def send_d(o, j):
        i = jnp.maximum(j - (units - ALONE - 1), 0)
        return pltpu.make_async_remote_copy(
            src_ref=dsend.at[o - 1, rows_of(j)], dst_ref=drecv.at[o - 1, rows_of(j)],
            send_sem=s_sem.at[0], recv_sem=d_sem.at[o - 1, i],
            device_id=device(t=opposite(o)), device_id_type=MESH,
        )

    def lend_u(o, j):
        return pltpu.make_async_remote_copy(
            src_ref=dsend.at[o - 1, rows_of(j)], dst_ref=lu.at[o - 1, rows_of(j)],
            send_sem=s_sem.at[0], recv_sem=l_sem.at[0],
            device_id=device(d=mate, t=opposite(o)), device_id_type=MESH,
        )

    def lend_g(j):
        return pltpu.make_async_remote_copy(
            src_ref=dg.at[rows_of(j)], dst_ref=lg.at[rows_of(j)],
            send_sem=u_send.at[0], recv_sem=l_sem.at[0],
            device_id=device(d=mate), device_id_type=MESH,
        )

    def lend_mask():
        return pltpu.make_async_remote_copy(
            src_ref=mask, dst_ref=lmask.at[0],
            send_sem=u_send.at[1], recv_sem=l_sem.at[2],
            device_id=device(d=mate), device_id_type=MESH,
        )

    given = rows_of(LENT, GIVEN)

    def give_u(o):
        return pltpu.make_async_remote_copy(
            src_ref=dsend.at[o - 1, given], dst_ref=ru.at[o - 1],
            send_sem=s_sem.at[0], recv_sem=r_sem.at[o],
            device_id=device(e=1), device_id_type=MESH,
        )

    def give_g():
        return pltpu.make_async_remote_copy(
            src_ref=dg.at[given], dst_ref=hg,
            send_sem=u_send.at[0], recv_sem=r_sem.at[0],
            device_id=device(e=1), device_id_type=MESH,
        )

    def pass_on(o, i):
        return pltpu.make_async_remote_copy(
            src_ref=ru.at[o - 1, rows_of(i)], dst_ref=hu.at[o - 1, rows_of(i)],
            send_sem=u_send.at[0], recv_sem=hu_sem.at[o - 1, i // (GIVEN - 1)],
            device_id=device(t=opposite(o)), device_id_type=MESH,
        )

    def pass_over_u(o):
        return pltpu.make_async_remote_copy(
            src_ref=dsend.at[o - 1, rows_of(FIRST, OVER)], dst_ref=yru.at[o - 1],
            send_sem=s_sem.at[0], recv_sem=y_sem.at[o - 1],
            device_id=device(d=place * stride), device_id_type=MESH,
        )

    def pass_over_g():
        return pltpu.make_async_remote_copy(
            src_ref=dg.at[rows_of(FIRST, OVER)], dst_ref=yhg, send_sem=u_send.at[0], recv_sem=l_sem.at[1],
            device_id=device(d=place * stride), device_id_type=MESH,
        )

    def pass_over_mask():
        return pltpu.make_async_remote_copy(
            src_ref=mask, dst_ref=lmask.at[1], send_sem=u_send.at[1], recv_sem=l_sem.at[2],
            device_id=device(d=place * stride), device_id_type=MESH,
        )

    def pass_through(o):
        return pltpu.make_async_remote_copy(
            src_ref=yru.at[o - 1], dst_ref=yhu.at[o - 1],
            send_sem=u_send.at[0], recv_sem=l_sem.at[1],
            device_id=device(t=opposite(o)), device_id_type=MESH,
        )

    def send_e(o, m, e0, count):
        part = pl.ds(e0 * qc, count * qc)
        return pltpu.make_async_remote_copy(
            src_ref=esend.at[o - 1, m, part], dst_ref=erecv.at[o - 1, m, part],
            send_sem=s_sem.at[1], recv_sem=e_sem,
            device_id=device(t=opposite(o)), device_id_type=MESH,
        )

    def landed(ref, sem):
        pltpu.make_async_copy(ref, ref, sem).wait()

    def signal(sem, who):
        pl.semaphore_signal(sem, inc=1, device_id=who, device_id_type=MESH)

    def tell_tensor(sem):
        for o in range(1, nt):
            signal(sem, device(t=opposite(o)))

    def tell_row(sem):
        for j in range(1, stride):
            signal(sem, device(d=place * stride + lax.rem(row + j, stride)))

    def tell_line(sem):
        @pl.when(place > 0)
        def _():
            signal(sem, device(d=dp - stride))

        @pl.when(place < places - 1)
        def _():
            signal(sem, device(d=dp + stride))

    on_line = (place > 0).astype(jnp.int32) + (place < places - 1).astype(jnp.int32)
    line_rounds = places - 1

    def hear_line(r):
        if r < line_rounds:
            pl.semaphore_wait(line_sem.at[r % 2], on_line)

    def next_line(r):
        if r < line_rounds:
            tell_line(line_sem.at[r % 2])

    w_epin.start()
    for o in range(1, nt):
        load_ea(o, 0, 1, 0).start()
    barrier = pltpu.get_barrier_semaphore()
    tell_tensor(barrier)
    for j in range(1, ne):
        signal(barrier, device(e=lax.rem(ex + j, ne)))
    tell_row(barrier)
    tell_line(barrier)
    for o in range(1, nt):
        load_ea(o, 1, micro - 1, 1).start()
    w_pin.start()
    acc[...] = jnp.zeros_like(acc)

    def expert_out(o, m, e0, count):
        esend[o - 1, m, pl.ds(e0 * qc, count * qc)] = jnp.dot(
            vea[o, m, pl.ds(e0, count)].reshape(count * qc, hidden), vepin[...], preferred_element_type=jnp.float32
        )

    half = max(experts // 2, 1)
    w_epin.wait()
    for o in range(1, nt):
        load_ea(o, 0, 1, 0).wait()
        expert_out(o, 0, 0, half)
    w_ids.start()
    pl.semaphore_wait(barrier, nt - 1 + ne - 1 + stride - 1 + on_line)
    for o in range(1, nt):
        send_e(o, 0, 0, half).start()
    for l in range(layers):
        for o in range(1, nt):
            load_a(o, l).start()
    w_pout.start()
    next_line(0)
    if half < experts:
        for o in range(1, nt):
            expert_out(o, 0, half, experts - half)
            send_e(o, 0, half, experts - half).start()
    for o in range(1, nt):
        load_ea(o, 1, micro - 1, 1).wait()

    @pl.loop(1, micro)
    def _(m):
        for o in range(1, nt):
            expert_out(o, m, 0, experts)
            send_e(o, m, 0, experts).start()

    w_pin.wait()
    w_dval.start()
    hear_line(0)
    next_line(1)
    for l in range(layers):
        for o in range(1, nt):
            load_a(o, l).wait()
        load_a(0, l).start()
        load_c(l).start()
        if l == layers - 1:
            hear_line(1)
            next_line(2)

        for first in range(0, micro, batch):
            for o in range(1, nt):
                dsend[o - 1, pl.ds((l * micro + first) * q, batch * q)] = jnp.dot(
                    va[o * layers + l, first : first + batch].reshape(batch * q, pin.shape[1]), vpin[l],
                    preferred_element_type=jnp.float32,
                )

            @pl.loop(0, batch * PIECES)
            def _(i):
                j = (l * micro + first) * PIECES + i
                for o in range(1, nt):

                    @pl.when(~kept(j))
                    def _():
                        send_d(o, j).start()

                    @pl.when(giver & (j == FIRST - 1))
                    def _():
                        give_u(o).start()

    w_ids.wait()
    load_ea(0, 0, micro, 0).start()
    load_ec.start()

    @pl.when(helper)
    def _():
        for o in range(1, nt):
            landed(ru.at[o - 1], r_sem.at[o])
            for i in range(GIVEN):
                pass_on(o, i).start()

    hear_line(2)
    for r in range(3, line_rounds):
        next_line(r)
        hear_line(r)
    tell_row(row_sem)
    w_pout.wait()
    w_dval.wait()
    w_epout.start()
    w_eval.start()

    lanes = rows.shape[2]
    lane = lax.broadcasted_iota(jnp.int32, (1, lanes), 1)

    def domain_of(m):
        return jnp.where(lane == vids[m], 1.0, 0.0)

    for j in range(LENT):
        mask[j] = domain_of(j // PIECES % micro)
    for j in range(FIRST, CROWD):
        mask[j - GIVEN] = domain_of(j // PIECES % micro)

    @pl.when(lent > 0)
    def _():
        lend_mask().start()
        for j in range(LENT):

            @pl.when(j < lent)
            def _():
                for o in range(1, nt):
                    lend_u(o, j).start()

    @pl.when(over)
    def _():
        pass_over_mask().start()
        for o in range(1, nt):
            pass_over_u(o).start()

    def fold(m, value):
        acc[m] += jnp.sum(value.reshape(-1, 8, rank), axis=0)

    def folds(some, value):
        acc[some] += jnp.sum(value.reshape(batch, -1, 8, rank), axis=1)

    for l in range(layers):
        landed(va.at[pl.ds(0, 1 + dim // act.shape[3])], a_sem.at[l])
        if l == layers - 1:
            pl.semaphore_wait(row_sem, stride - 1)
            tell_tensor(tensor_sem)

        for first in range(0, micro, batch):
            some = slice(first, first + batch)
            u = jnp.dot(
                va[l, some].reshape(batch * q, pin.shape[1]), vpin[l], preferred_element_type=jnp.float32
            )
            w = jnp.dot(vc[l, some].reshape(batch * q, dim), vpout[l], preferred_element_type=jnp.float32)
            g = lax.dot_general(
                w, vdv[l], (((1,), (1,)), ((), ())), precision=HIGHEST, preferred_element_type=jnp.float32
            )
            dg[pl.ds((l * micro + first) * q, batch * q)] = g
            folds(some, u * g)
            done = range((l * micro + first) * PIECES, (l * micro + first + batch) * PIECES)
            for j in range(LENT):
                if j in done:

                    @pl.when(j < lent)
                    def _():
                        lend_g(j).start()

            if FIRST - 1 in done:

                @pl.when(giver)
                def _():
                    give_g().start()

            if CROWD - 1 in done:

                @pl.when(over)
                def _():
                    pass_over_g().start()

    w_epout.wait()
    w_eval.wait()
    w_prior.start()
    load_ea(0, 0, micro, 0).wait()
    load_ec.wait()
    pl.semaphore_wait(tensor_sem, nt - 1)

    for first in range(0, micro, batch):
        some = slice(first, first + batch)
        u = jnp.dot(
            vea[0, some].reshape(batch * experts * qc, hidden), vepin[...], preferred_element_type=jnp.float32
        )
        w = jnp.dot(vec[some].reshape(batch * experts * qc, dim), vepout[...], preferred_element_type=jnp.float32)
        w = w.reshape(batch, experts, qc, rank)
        g = [
            lax.dot_general(
                w[:, e].reshape(batch * qc, rank), vev[e], (((1,), (1,)), ((), ())),
                precision=HIGHEST, preferred_element_type=jnp.float32,
            ).reshape(batch, 1, qc, rank)
            for e in range(experts)
        ]
        g = jnp.concatenate(g, axis=1).reshape(batch, experts * qc, rank)
        eg[some] = g
        folds(some, u.reshape(batch, experts * qc, rank) * g)
        if first == 0:

            @pl.when(guest)
            def _():
                for o in range(1, nt):
                    landed(yru.at[o - 1], y_sem.at[o - 1])
                    pass_through(o).start()

    landed(erecv, e_sem)

    @pl.loop(0, micro)
    def _(m):
        for o in range(1, nt):
            fold(m, erecv[o - 1, m] * eg[m])

    w_prior.wait()

    def cross(o, j, count=1):
        return drecv[o - 1, rows_of(j, count)] * dg[rows_of(j, count)]

    def total_of(value):
        return jnp.sum(jnp.sum(value, axis=1, keepdims=True), axis=0, keepdims=True)

    rows[me] = jnp.zeros((1, lanes), jnp.float32)

    masks = count_of(taken > 0) + count_of(guest)
    for c in (1, 2):

        @pl.when(masks == c)
        def _():
            landed(lmask.at[pl.ds(0, c)], l_sem.at[2])

    @pl.when(taken > 0)
    def _():
        for c in range(1, LENT + 1):

            @pl.when(taken == c)
            def _():
                landed(drecv.at[0, rows_of(0, nt * c)], l_sem.at[0])

        for j in range(LENT):

            @pl.when(j < taken)
            def _():
                value = jnp.zeros((8, rank), jnp.float32)
                for o in range(1, nt):
                    both = lu[o - 1, rows_of(j)] * lg[rows_of(j)]
                    value = value + jnp.sum(both.reshape(-1, 8, rank), axis=0)
                rows[me] += lmask[0, j] * total_of(value)

    together = units - ALONE - lent - GIVEN * count_of(giver) - OVER * count_of(over)
    for c in range(units - ALONE - CROWD, units - ALONE + 1):

        @pl.when(together == c)
        def _():
            for o in range(1, nt):
                landed(drecv.at[o - 1, rows_of(0, c)], d_sem.at[o - 1, 0])

    full = -(-CROWD // PIECES)
    for j in [*range(full * PIECES), *range((blocks - 1) * PIECES, units - ALONE)]:

        @pl.when(~kept(j))
        def _():
            for o in range(1, nt):
                fold(j // PIECES % micro, cross(o, j))

    @pl.loop(full, blocks - 1)
    def _(k):
        for o in range(1, nt):
            fold(lax.rem(k, micro), cross(o, k * PIECES, PIECES))

    def take(o, j):
        landed(drecv.at[o - 1, rows_of(j)], d_sem.at[o - 1, j - units + ALONE + 1])

    def take_given(o, i):
        return hu[o - 1, rows_of(i)] * hg[rows_of(i)]

    def shorter(value):
        return jnp.sum(value.reshape(-1, 8, rank), axis=0)

    last = [(o, j) for j in range(units - ALONE, units) for o in range(1, nt)]
    for o, j in last[:-1]:
        take(o, j)
        fold(j // PIECES % micro, cross(o, j))
    o, j = last[-1]

    @pl.when(guest)
    def _():
        landed(drecv.at[0, rows_of(0, nt * OVER)], l_sem.at[1])
        for i in range(OVER):
            value = jnp.zeros((8, rank), jnp.float32)
            for o_ in range(1, nt):
                value = value + shorter(yhu[o_ - 1, rows_of(i)] * yhg[rows_of(i)])
            rows[me] += lmask[1, LENT + i] * total_of(value)

    @pl.when(helper)
    def _():
        take(o, j)
        fold(micro - 1, cross(o, j))
        landed(hg, r_sem.at[0])
        for o_ in range(1, nt):
            landed(hu.at[o_ - 1, rows_of(0, GIVEN - 1)], hu_sem.at[o_ - 1, 0])
            for i in range(GIVEN - 1):
                fold((LENT + i) // PIECES % micro, take_given(o_, i))
        for o_ in range(1, nt - 1):
            landed(hu.at[o_ - 1, rows_of(GIVEN - 1)], hu_sem.at[o_ - 1, 1])
            fold((FIRST - 1) // PIECES % micro, take_given(o_, GIVEN - 1))

    part = rows[me]
    for m in range(micro):
        part = part + domain_of(m) * total_of(acc[m])
    rows[me] = part
    chosen = jnp.where(helper, domain_of((FIRST - 1) // PIECES % micro), domain_of(micro - 1))

    @pl.when(helper)
    def _():
        landed(hu.at[nt - 2, rows_of(GIVEN - 1)], hu_sem.at[nt - 2, 1])
        fin[...] = shorter(take_given(nt - 1, GIVEN - 1))

    @pl.when(~helper)
    def _():
        take(o, j)
        fin[...] = shorter(cross(o, j))

    rows[me] += chosen * total_of(fin[...])

    for i in range(n - 1):
        pltpu.make_async_remote_copy(
            src_ref=rows.at[me], dst_ref=rows.at[me], send_sem=row_send, recv_sem=row_recv,
            device_id=i + (me <= i).astype(jnp.int32), device_id_type=LOGICAL,
        ).start()

    for o in range(1, nt):
        landed(dsend.at[o - 1], s_sem.at[0])
    landed(esend, s_sem.at[1])

    masks = count_of(lent > 0) + count_of(over)
    for c in (1, 2):

        @pl.when(masks == c)
        def _():
            landed(lmask.at[pl.ds(0, c)], u_send.at[1])

    sent = lent + GIVEN * (count_of(giver) + (nt - 1) * count_of(helper))
    sent = sent + OVER * (count_of(over) + (nt - 1) * count_of(guest))
    for c in range(1, LENT + (nt - 1) * (GIVEN + OVER) + 1):

        @pl.when(sent == c)
        def _():
            landed(drecv.at[0, rows_of(0, c)], u_send.at[0])

    others = rows.at[pl.ds(0, n - 1)]
    landed(others, row_recv)
    domains = prior.shape[1]
    total = jnp.sum(rows[...], axis=0)[:, :domains]
    spread = jnp.sqrt(jnp.sum(total * total, axis=1, keepdims=True) * (1.0 / domains) + 1e-06)
    z = total / spread
    mix = vprior[...]
    mass = jnp.sum(mix * jnp.exp(0.5 * z), axis=1, keepdims=True)
    out[...] = jnp.log(mix) + 0.5 * z - jnp.log(mass)
    landed(others, row_send)


def per_device(sizes, *args):
    (act, cot, pin, pout, eact, ecot, epin, epout, dval, evals, ids, prior) = args
    nd, ne, nt = sizes
    n = nd * ne * nt
    places = line_of(nd)[1]
    layers, micro, q, dim = cot.shape
    rank, feat = pin.shape[2], pin.shape[1]
    experts, qc, hidden = ecot.shape[1], ecot.shape[2], eact.shape[3]
    domains = prior.shape[0]
    lanes = -(-domains // 128) * 128
    lent, given, over = (units * (q // PIECES) for units in (LENT, GIVEN, OVER))
    bf, f32 = jnp.bfloat16, jnp.float32
    V, dma, regular = pltpu.VMEM, pltpu.SemaphoreType.DMA, pltpu.SemaphoreType.REGULAR
    logs = pl.pallas_call(
        functools.partial(kernel, sizes),
        out_shape=pltpu.VMEM((1, domains), f32),
        in_specs=[pl.BlockSpec(memory_space=pltpu.HBM)] * 12,
        out_specs=pl.BlockSpec(memory_space=pltpu.VMEM),
        scratch_shapes=[
            V((nt * layers, micro, q, feat), bf),
            V((layers, micro, q, dim), bf),
            V(pin.shape, bf),
            V(pout.shape, bf),
            V((nt, micro, experts, qc, hidden), bf),
            V((micro, experts, qc, dim), bf),
            V(epin.shape, bf),
            V(epout.shape, bf),
            V(dval.shape, f32),
            V(evals.shape, f32),
            pltpu.SMEM(ids.shape, jnp.int32),
            V((1, domains), f32),
            V((nt - 1, layers * micro * q, rank), f32),
            V((nt - 1, layers * micro * q, rank), f32),
            V((nt - 1, micro, experts * qc, rank), f32),
            V((nt - 1, micro, experts * qc, rank), f32),
            V((layers * micro * q, rank), f32),
            V((micro, experts * qc, rank), f32),
            V((nt - 1, lent, rank), f32),
            V((lent, rank), f32),
            V((2, LENT + OVER, 1, lanes), f32),
            V((LENT + OVER, 1, lanes), f32),
            V((nt - 1, given, rank), f32),
            V((nt - 1, given, rank), f32),
            V((given, rank), f32),
            V((nt - 1, over, rank), f32),
            V((nt - 1, over, rank), f32),
            V((over, rank), f32),
            V((micro, 8, rank), f32),
            V((8, rank), f32),
            V((n, 1, lanes), f32),
            dma((layers,)),
            dma((2,)),
            dma((2,)),
            dma((2,)),
            dma,
            dma((nt - 1, 1 + ALONE)),
            dma((3,)),
            dma((2,)),
            dma((nt,)),
            dma((nt - 1, 2)),
            dma((nt - 1,)),
            dma,
            dma,
            regular((2,)),
            regular,
            regular,
        ],
        compiler_params=pltpu.CompilerParams(
            collective_id=0, has_side_effects=True, vmem_limit_bytes=60 * 1024 * 1024
        ),
        name="align",
    )(act, cot, pin, pout, eact, ecot, epin, epout, dval, evals, ids, prior.reshape(1, domains))
    share = domains // nd
    return lax.dynamic_slice_in_dim(logs[0], lax.axis_index("dp") * share, share, 0)


def solution(mesh):
    sizes = (mesh.shape["dp"], mesh.shape["expert"], mesh.shape["tensor"])
    placed = (
        P(None, "dp", "expert", "tensor"),
        P(None, "dp", ("expert", "tensor"), None),
        P(None, "tensor", None),
        P(),
        P("dp", "expert", None, "tensor"),
        P("dp", "expert", "tensor", None),
        P("tensor", None),
        P(),
        P(),
        P("expert", None, None),
        P("dp"),
        P(),
    )
    return jax.shard_map(
        functools.partial(per_device, sizes), mesh=mesh, in_specs=placed, out_specs=P("dp"), check_vma=False
    )
```

```python
import functools

import jax
import jax.numpy as jnp
from jax import lax
from jax.experimental import pallas as pl
from jax.experimental.pallas import tpu as pltpu
from jax.sharding import PartitionSpec as P

MESH, LOGICAL = pl.DeviceIdType.MESH, pl.DeviceIdType.LOGICAL
HIGHEST = lax.Precision.HIGHEST
BATCH = 2
PIECES = 4
LENT = 5
GIVEN = 7
OVER = 2
FIRST = LENT + GIVEN
CROWD = FIRST + OVER
ALONE = 2


def line_of(nd):
    stride = 2 if nd % 2 == 0 else 1
    return stride, nd // stride


def kernel(
    sizes,
    act, cot, pin, pout, eact, ecot, epin, epout, dval, evals, ids, prior,
    out,
    va, vc, vpin, vpout, vea, vec, vepin, vepout, vdv, vev, vids, vprior,
    dsend, drecv, esend, erecv, dg, eg, lu, lg, lmask, mask, ru, hu, hg, yru, yhu, yhg, acc, fin, rows,
    a_sem, ea_sem, w_sem, s_sem, e_sem, d_sem, l_sem, u_send, r_sem, hu_sem, y_sem, row_send, row_recv,
    line_sem, row_sem, tensor_sem,
):
    nd, ne, nt = sizes
    n = nd * ne * nt
    stride, places = line_of(nd)
    dp, ex, tx = lax.axis_index("dp"), lax.axis_index("expert"), lax.axis_index("tensor")
    me = (dp * ne + ex) * nt + tx
    place, row = lax.div(dp, stride), lax.rem(dp, stride)
    layers, micro, q, rank = cot.shape[0], cot.shape[1], cot.shape[2], pin.shape[2]
    experts, qc = ecot.shape[1], ecot.shape[2]
    hidden = eact.shape[3]
    dim = ecot.shape[3]
    h = q // PIECES
    blocks = layers * micro
    units = blocks * PIECES
    full = -(-CROWD // PIECES)
    batch = BATCH if micro % BATCH == 0 else 1
    mate = (places - 1 - place) * stride + row

    def lends(at):
        return jnp.where(2 * at >= places, jnp.clip(3 * (at + row - (places + stride) // 2 + 1) - row, 0, LENT), 0)

    lent, taken = lends(place), lends(places - 1 - place)
    near = 2 * place < places
    over, guest = ((row == 1) & near, (row == 0) & near) if stride > 1 else (row < 0, row < 0)
    giver, helper = (ex == 0, ex == 1) if ne > 1 else (ex < 0, ex < 0)

    def kept(j):
        return (j < lent) | (giver & (j >= LENT) & (j < FIRST)) | (over & (j >= FIRST) & (j < CROWD))

    def count_of(flag):
        return jnp.where(flag, 1, 0)

    def device(d=None, e=None, t=None):
        return {
            "dp": dp if d is None else d,
            "expert": ex if e is None else e,
            "tensor": tx if t is None else t,
        }

    def load_a(o, l):
        first = pl.multiple_of(lax.rem(tx + o, nt) * q, q)
        return pltpu.make_async_copy(act.at[l, :, pl.ds(first, q), :], va.at[o * layers + l], a_sem.at[l])

    def load_ea(o, first_m, count, i):
        first = pl.multiple_of(lax.rem(tx + o, nt) * qc, qc)
        some = pl.ds(first_m, count)
        return pltpu.make_async_copy(eact.at[some, :, pl.ds(first, qc), :], vea.at[o, some], ea_sem.at[i])

    def load_c(l):
        return pltpu.make_async_copy(cot.at[l], vc.at[l], a_sem.at[l])

    load_ec = pltpu.make_async_copy(ecot, vec, ea_sem.at[1])

    def load_w(src, dst, i):
        return pltpu.make_async_copy(src, dst, w_sem.at[i])

    w_epin, w_pout, w_epout = load_w(epin, vepin, 0), load_w(pout, vpout, 0), load_w(epout, vepout, 0)
    w_pin, w_dval, w_eval = load_w(pin, vpin, 1), load_w(dval, vdv, 1), load_w(evals, vev, 1)
    w_ids, w_prior = pltpu.make_async_copy(ids, vids, ea_sem.at[0]), load_w(prior, vprior, 0)

    def rows_of(j, count=1):
        return pl.ds(pl.multiple_of(j * h, h), count * h)

    def opposite(o):
        return lax.rem(tx + o, nt)

    def send_d(o, j, count=1):
        i = jnp.maximum(j - (units - ALONE - 1), 0)
        return pltpu.make_async_remote_copy(
            src_ref=dsend.at[o - 1, rows_of(j, count)], dst_ref=drecv.at[o - 1, rows_of(j, count)],
            send_sem=s_sem.at[0], recv_sem=d_sem.at[o - 1, i],
            device_id=device(t=opposite(o)), device_id_type=MESH,
        )

    def lend_u(o, j):
        return pltpu.make_async_remote_copy(
            src_ref=dsend.at[o - 1, rows_of(j)], dst_ref=lu.at[o - 1, rows_of(j)],
            send_sem=s_sem.at[0], recv_sem=l_sem.at[0],
            device_id=device(d=mate, t=opposite(o)), device_id_type=MESH,
        )

    def lend_g(j):
        return pltpu.make_async_remote_copy(
            src_ref=dg.at[rows_of(j)], dst_ref=lg.at[rows_of(j)],
            send_sem=u_send.at[0], recv_sem=l_sem.at[0],
            device_id=device(d=mate), device_id_type=MESH,
        )

    def lend_mask():
        return pltpu.make_async_remote_copy(
            src_ref=mask, dst_ref=lmask.at[0],
            send_sem=u_send.at[1], recv_sem=l_sem.at[2],
            device_id=device(d=mate), device_id_type=MESH,
        )

    given = rows_of(LENT, GIVEN)

    def give_u(o):
        return pltpu.make_async_remote_copy(
            src_ref=dsend.at[o - 1, given], dst_ref=ru.at[o - 1],
            send_sem=s_sem.at[0], recv_sem=r_sem.at[o],
            device_id=device(e=1), device_id_type=MESH,
        )

    def give_g():
        return pltpu.make_async_remote_copy(
            src_ref=dg.at[given], dst_ref=hg,
            send_sem=u_send.at[0], recv_sem=r_sem.at[0],
            device_id=device(e=1), device_id_type=MESH,
        )

    def pass_on(o, i):
        return pltpu.make_async_remote_copy(
            src_ref=ru.at[o - 1, rows_of(i)], dst_ref=hu.at[o - 1, rows_of(i)],
            send_sem=u_send.at[0], recv_sem=hu_sem.at[o - 1, i // (GIVEN - 1)],
            device_id=device(t=opposite(o)), device_id_type=MESH,
        )

    def pass_over_u(o):
        return pltpu.make_async_remote_copy(
            src_ref=dsend.at[o - 1, rows_of(FIRST, OVER)], dst_ref=yru.at[o - 1],
            send_sem=s_sem.at[0], recv_sem=y_sem.at[o - 1],
            device_id=device(d=place * stride), device_id_type=MESH,
        )

    def pass_over_g():
        return pltpu.make_async_remote_copy(
            src_ref=dg.at[rows_of(FIRST, OVER)], dst_ref=yhg, send_sem=u_send.at[0], recv_sem=l_sem.at[1],
            device_id=device(d=place * stride), device_id_type=MESH,
        )

    def pass_over_mask():
        return pltpu.make_async_remote_copy(
            src_ref=mask, dst_ref=lmask.at[1], send_sem=u_send.at[1], recv_sem=l_sem.at[2],
            device_id=device(d=place * stride), device_id_type=MESH,
        )

    def pass_through(o):
        return pltpu.make_async_remote_copy(
            src_ref=yru.at[o - 1], dst_ref=yhu.at[o - 1],
            send_sem=u_send.at[0], recv_sem=l_sem.at[1],
            device_id=device(t=opposite(o)), device_id_type=MESH,
        )

    def send_e(o, m, e0, count):
        part = pl.ds(e0 * qc, count * qc)
        return pltpu.make_async_remote_copy(
            src_ref=esend.at[o - 1, m, part], dst_ref=erecv.at[o - 1, m, part],
            send_sem=s_sem.at[1], recv_sem=e_sem,
            device_id=device(t=opposite(o)), device_id_type=MESH,
        )

    def landed(ref, sem):
        pltpu.make_async_copy(ref, ref, sem).wait()

    def signal(sem, who):
        pl.semaphore_signal(sem, inc=1, device_id=who, device_id_type=MESH)

    def tell_tensor(sem):
        for o in range(1, nt):
            signal(sem, device(t=opposite(o)))

    def tell_row(sem):
        for j in range(1, stride):
            signal(sem, device(d=place * stride + lax.rem(row + j, stride)))

    def tell_line(sem):
        @pl.when(place > 0)
        def _():
            signal(sem, device(d=dp - stride))

        @pl.when(place < places - 1)
        def _():
            signal(sem, device(d=dp + stride))

    on_line = (place > 0).astype(jnp.int32) + (place < places - 1).astype(jnp.int32)
    line_rounds = places - 1

    def hear_line(r):
        if r < line_rounds:
            pl.semaphore_wait(line_sem.at[r % 2], on_line)

    def next_line(r):
        if r < line_rounds:
            tell_line(line_sem.at[r % 2])

    w_epin.start()
    for o in range(1, nt):
        load_ea(o, 0, 1, 0).start()
    barrier = pltpu.get_barrier_semaphore()
    tell_tensor(barrier)
    for j in range(1, ne):
        signal(barrier, device(e=lax.rem(ex + j, ne)))
    tell_row(barrier)
    tell_line(barrier)
    for o in range(1, nt):
        load_ea(o, 1, micro - 1, 1).start()
    w_pin.start()
    acc[...] = jnp.zeros_like(acc)

    def expert_out(o, m, e0, count):
        esend[o - 1, m, pl.ds(e0 * qc, count * qc)] = jnp.dot(
            vea[o, m, pl.ds(e0, count)].reshape(count * qc, hidden), vepin[...], preferred_element_type=jnp.float32
        )

    half = max(experts // 2, 1)
    w_epin.wait()
    for o in range(1, nt):
        load_ea(o, 0, 1, 0).wait()
        expert_out(o, 0, 0, half)
    w_ids.start()
    pl.semaphore_wait(barrier, nt - 1 + ne - 1 + stride - 1 + on_line)
    for o in range(1, nt):
        send_e(o, 0, 0, half).start()
    for l in range(layers):
        for o in range(1, nt):
            load_a(o, l).start()
    w_pout.start()
    next_line(0)
    if half < experts:
        for o in range(1, nt):
            expert_out(o, 0, half, experts - half)
            send_e(o, 0, half, experts - half).start()
    for o in range(1, nt):
        load_ea(o, 1, micro - 1, 1).wait()

    @pl.loop(1, micro)
    def _(m):
        for o in range(1, nt):
            expert_out(o, m, 0, experts)
            send_e(o, m, 0, experts).start()

    w_pin.wait()
    w_dval.start()
    hear_line(0)
    next_line(1)
    for l in range(layers):
        for o in range(1, nt):
            load_a(o, l).wait()
        load_a(0, l).start()
        load_c(l).start()
        if l == layers - 1:
            hear_line(1)
            next_line(2)

        for first in range(0, micro, batch):
            for o in range(1, nt):
                dsend[o - 1, pl.ds((l * micro + first) * q, batch * q)] = jnp.dot(
                    va[o * layers + l, first : first + batch].reshape(batch * q, pin.shape[1]), vpin[l],
                    preferred_element_type=jnp.float32,
                )

            @pl.loop(0, batch * PIECES)
            def _(i):
                j = (l * micro + first) * PIECES + i
                for o in range(1, nt):

                    whole = (j >= full * PIECES) & (j < (blocks - 1) * PIECES)

                    @pl.when(whole & (lax.rem(j, PIECES) == 0))
                    def _():
                        send_d(o, j, PIECES).start()

                    @pl.when(~(whole | kept(j)))
                    def _():
                        send_d(o, j).start()

                    @pl.when(giver & (j == FIRST - 1))
                    def _():
                        give_u(o).start()

    w_ids.wait()
    load_ea(0, 0, micro, 0).start()
    load_ec.start()

    @pl.when(helper)
    def _():
        for o in range(1, nt):
            landed(ru.at[o - 1], r_sem.at[o])
            for i in range(GIVEN):
                pass_on(o, i).start()

    hear_line(2)
    for r in range(3, line_rounds):
        next_line(r)
        hear_line(r)
    tell_row(row_sem)
    w_pout.wait()
    w_dval.wait()
    w_epout.start()
    w_eval.start()

    lanes = rows.shape[2]
    lane = lax.broadcasted_iota(jnp.int32, (1, lanes), 1)

    def domain_of(m):
        return jnp.where(lane == vids[m], 1.0, 0.0)

    for j in range(LENT):
        mask[j] = domain_of(j // PIECES % micro)
    for j in range(FIRST, CROWD):
        mask[j - GIVEN] = domain_of(j // PIECES % micro)

    @pl.when(lent > 0)
    def _():
        lend_mask().start()
        for j in range(LENT):

            @pl.when(j < lent)
            def _():
                for o in range(1, nt):
                    lend_u(o, j).start()

    @pl.when(over)
    def _():
        pass_over_mask().start()
        for o in range(1, nt):
            pass_over_u(o).start()

    def fold(m, value):
        acc[m] += jnp.sum(value.reshape(-1, 8, rank), axis=0)

    def folds(some, value):
        acc[some] += jnp.sum(value.reshape(batch, -1, 8, rank), axis=1)

    for l in range(layers):
        landed(va.at[pl.ds(0, 1 + dim // act.shape[3])], a_sem.at[l])
        if l == layers - 1:
            pl.semaphore_wait(row_sem, stride - 1)
            tell_tensor(tensor_sem)

        for first in range(0, micro, batch):
            some = slice(first, first + batch)
            u = jnp.dot(
                va[l, some].reshape(batch * q, pin.shape[1]), vpin[l], preferred_element_type=jnp.float32
            )
            w = jnp.dot(vc[l, some].reshape(batch * q, dim), vpout[l], preferred_element_type=jnp.float32)
            g = lax.dot_general(
                w, vdv[l], (((1,), (1,)), ((), ())), precision=HIGHEST, preferred_element_type=jnp.float32
            )
            dg[pl.ds((l * micro + first) * q, batch * q)] = g
            folds(some, u * g)
            done = range((l * micro + first) * PIECES, (l * micro + first + batch) * PIECES)
            for j in range(LENT):
                if j in done:

                    @pl.when(j < lent)
                    def _():
                        lend_g(j).start()

            if FIRST - 1 in done:

                @pl.when(giver)
                def _():
                    give_g().start()

            if CROWD - 1 in done:

                @pl.when(over)
                def _():
                    pass_over_g().start()

    w_epout.wait()
    w_eval.wait()
    w_prior.start()
    load_ea(0, 0, micro, 0).wait()
    load_ec.wait()
    pl.semaphore_wait(tensor_sem, nt - 1)

    for first in range(0, micro, batch):
        some = slice(first, first + batch)
        u = jnp.dot(
            vea[0, some].reshape(batch * experts * qc, hidden), vepin[...], preferred_element_type=jnp.float32
        )
        w = jnp.dot(vec[some].reshape(batch * experts * qc, dim), vepout[...], preferred_element_type=jnp.float32)
        w = w.reshape(batch, experts, qc, rank)
        g = [
            lax.dot_general(
                w[:, e].reshape(batch * qc, rank), vev[e], (((1,), (1,)), ((), ())),
                precision=HIGHEST, preferred_element_type=jnp.float32,
            ).reshape(batch, 1, qc, rank)
            for e in range(experts)
        ]
        g = jnp.concatenate(g, axis=1).reshape(batch, experts * qc, rank)
        eg[some] = g
        folds(some, u.reshape(batch, experts * qc, rank) * g)
        if first == 0:

            @pl.when(guest)
            def _():
                for o in range(1, nt):
                    landed(yru.at[o - 1], y_sem.at[o - 1])
                    pass_through(o).start()

    landed(erecv, e_sem)

    @pl.loop(0, micro)
    def _(m):
        for o in range(1, nt):
            fold(m, erecv[o - 1, m] * eg[m])

    w_prior.wait()

    def cross(o, j, count=1):
        return drecv[o - 1, rows_of(j, count)] * dg[rows_of(j, count)]

    def total_of(value):
        return jnp.sum(jnp.sum(value, axis=1, keepdims=True), axis=0, keepdims=True)

    rows[me] = jnp.zeros((1, lanes), jnp.float32)

    masks = count_of(taken > 0) + count_of(guest)
    for c in (1, 2):

        @pl.when(masks == c)
        def _():
            landed(lmask.at[pl.ds(0, c)], l_sem.at[2])

    @pl.when(taken > 0)
    def _():
        for c in range(1, LENT + 1):

            @pl.when(taken == c)
            def _():
                landed(drecv.at[0, rows_of(0, nt * c)], l_sem.at[0])

        for j in range(LENT):

            @pl.when(j < taken)
            def _():
                value = jnp.zeros((8, rank), jnp.float32)
                for o in range(1, nt):
                    both = lu[o - 1, rows_of(j)] * lg[rows_of(j)]
                    value = value + jnp.sum(both.reshape(-1, 8, rank), axis=0)
                rows[me] += lmask[0, j] * total_of(value)

    together = units - ALONE - lent - GIVEN * count_of(giver) - OVER * count_of(over)
    for c in range(units - ALONE - CROWD, units - ALONE + 1):

        @pl.when(together == c)
        def _():
            for o in range(1, nt):
                landed(drecv.at[o - 1, rows_of(0, c)], d_sem.at[o - 1, 0])

    for j in [*range(full * PIECES), *range((blocks - 1) * PIECES, units - ALONE)]:

        @pl.when(~kept(j))
        def _():
            for o in range(1, nt):
                fold(j // PIECES % micro, cross(o, j))

    @pl.loop(full, blocks - 1)
    def _(k):
        for o in range(1, nt):
            fold(lax.rem(k, micro), cross(o, k * PIECES, PIECES))

    def take(o, j):
        landed(drecv.at[o - 1, rows_of(j)], d_sem.at[o - 1, j - units + ALONE + 1])

    def take_given(o, i):
        return hu[o - 1, rows_of(i)] * hg[rows_of(i)]

    def shorter(value):
        return jnp.sum(value.reshape(-1, 8, rank), axis=0)

    last = [(o, j) for j in range(units - ALONE, units) for o in range(1, nt)]
    for o, j in last[:-1]:
        take(o, j)
        fold(j // PIECES % micro, cross(o, j))
    o, j = last[-1]

    @pl.when(guest)
    def _():
        landed(drecv.at[0, rows_of(0, nt * OVER)], l_sem.at[1])
        for i in range(OVER):
            value = jnp.zeros((8, rank), jnp.float32)
            for o_ in range(1, nt):
                value = value + shorter(yhu[o_ - 1, rows_of(i)] * yhg[rows_of(i)])
            rows[me] += lmask[1, LENT + i] * total_of(value)

    @pl.when(helper)
    def _():
        take(o, j)
        fold(micro - 1, cross(o, j))
        landed(hg, r_sem.at[0])
        for o_ in range(1, nt):
            landed(hu.at[o_ - 1, rows_of(0, GIVEN - 1)], hu_sem.at[o_ - 1, 0])
            for i in range(GIVEN - 1):
                fold((LENT + i) // PIECES % micro, take_given(o_, i))
        for o_ in range(1, nt - 1):
            landed(hu.at[o_ - 1, rows_of(GIVEN - 1)], hu_sem.at[o_ - 1, 1])
            fold((FIRST - 1) // PIECES % micro, take_given(o_, GIVEN - 1))

    part = rows[me]
    for m in range(micro):
        part = part + domain_of(m) * total_of(acc[m])
    rows[me] = part
    chosen = jnp.where(helper, domain_of((FIRST - 1) // PIECES % micro), domain_of(micro - 1))

    @pl.when(helper)
    def _():
        landed(hu.at[nt - 2, rows_of(GIVEN - 1)], hu_sem.at[nt - 2, 1])
        fin[...] = shorter(take_given(nt - 1, GIVEN - 1))

    @pl.when(~helper)
    def _():
        take(o, j)
        fin[...] = shorter(cross(o, j))

    rows[me] += chosen * total_of(fin[...])

    for i in range(n - 1):
        pltpu.make_async_remote_copy(
            src_ref=rows.at[me], dst_ref=rows.at[me], send_sem=row_send, recv_sem=row_recv,
            device_id=i + (me <= i).astype(jnp.int32), device_id_type=LOGICAL,
        ).start()

    for o in range(1, nt):
        landed(dsend.at[o - 1], s_sem.at[0])
    landed(esend, s_sem.at[1])

    masks = count_of(lent > 0) + count_of(over)
    for c in (1, 2):

        @pl.when(masks == c)
        def _():
            landed(lmask.at[pl.ds(0, c)], u_send.at[1])

    sent = lent + GIVEN * (count_of(giver) + (nt - 1) * count_of(helper))
    sent = sent + OVER * (count_of(over) + (nt - 1) * count_of(guest))
    for c in range(1, LENT + (nt - 1) * (GIVEN + OVER) + 1):

        @pl.when(sent == c)
        def _():
            landed(drecv.at[0, rows_of(0, c)], u_send.at[0])

    others = rows.at[pl.ds(0, n - 1)]
    landed(others, row_recv)
    domains = prior.shape[1]
    total = jnp.sum(rows[...], axis=0)[:, :domains]
    spread = jnp.sqrt(jnp.sum(total * total, axis=1, keepdims=True) * (1.0 / domains) + 1e-06)
    z = total / spread
    mix = vprior[...]
    mass = jnp.sum(mix * jnp.exp(0.5 * z), axis=1, keepdims=True)
    out[...] = jnp.log(mix) + 0.5 * z - jnp.log(mass)
    landed(others, row_send)


def per_device(sizes, *args):
    (act, cot, pin, pout, eact, ecot, epin, epout, dval, evals, ids, prior) = args
    nd, ne, nt = sizes
    n = nd * ne * nt
    places = line_of(nd)[1]
    layers, micro, q, dim = cot.shape
    rank, feat = pin.shape[2], pin.shape[1]
    experts, qc, hidden = ecot.shape[1], ecot.shape[2], eact.shape[3]
    domains = prior.shape[0]
    lanes = -(-domains // 128) * 128
    lent, given, over = (units * (q // PIECES) for units in (LENT, GIVEN, OVER))
    bf, f32 = jnp.bfloat16, jnp.float32
    V, dma, regular = pltpu.VMEM, pltpu.SemaphoreType.DMA, pltpu.SemaphoreType.REGULAR
    logs = pl.pallas_call(
        functools.partial(kernel, sizes),
        out_shape=pltpu.VMEM((1, domains), f32),
        in_specs=[pl.BlockSpec(memory_space=pltpu.HBM)] * 12,
        out_specs=pl.BlockSpec(memory_space=pltpu.VMEM),
        scratch_shapes=[
            V((nt * layers, micro, q, feat), bf),
            V((layers, micro, q, dim), bf),
            V(pin.shape, bf),
            V(pout.shape, bf),
            V((nt, micro, experts, qc, hidden), bf),
            V((micro, experts, qc, dim), bf),
            V(epin.shape, bf),
            V(epout.shape, bf),
            V(dval.shape, f32),
            V(evals.shape, f32),
            pltpu.SMEM(ids.shape, jnp.int32),
            V((1, domains), f32),
            V((nt - 1, layers * micro * q, rank), f32),
            V((nt - 1, layers * micro * q, rank), f32),
            V((nt - 1, micro, experts * qc, rank), f32),
            V((nt - 1, micro, experts * qc, rank), f32),
            V((layers * micro * q, rank), f32),
            V((micro, experts * qc, rank), f32),
            V((nt - 1, lent, rank), f32),
            V((lent, rank), f32),
            V((2, LENT + OVER, 1, lanes), f32),
            V((LENT + OVER, 1, lanes), f32),
            V((nt - 1, given, rank), f32),
            V((nt - 1, given, rank), f32),
            V((given, rank), f32),
            V((nt - 1, over, rank), f32),
            V((nt - 1, over, rank), f32),
            V((over, rank), f32),
            V((micro, 8, rank), f32),
            V((8, rank), f32),
            V((n, 1, lanes), f32),
            dma((layers,)),
            dma((2,)),
            dma((2,)),
            dma((2,)),
            dma,
            dma((nt - 1, 1 + ALONE)),
            dma((3,)),
            dma((2,)),
            dma((nt,)),
            dma((nt - 1, 2)),
            dma((nt - 1,)),
            dma,
            dma,
            regular((2,)),
            regular,
            regular,
        ],
        compiler_params=pltpu.CompilerParams(
            collective_id=0, has_side_effects=True, vmem_limit_bytes=60 * 1024 * 1024
        ),
        name="align",
    )(act, cot, pin, pout, eact, ecot, epin, epout, dval, evals, ids, prior.reshape(1, domains))
    share = domains // nd
    return lax.dynamic_slice_in_dim(logs[0], lax.axis_index("dp") * share, share, 0)


def solution(mesh):
    sizes = (mesh.shape["dp"], mesh.shape["expert"], mesh.shape["tensor"])
    placed = (
        P(None, "dp", "expert", "tensor"),
        P(None, "dp", ("expert", "tensor"), None),
        P(None, "tensor", None),
        P(),
        P("dp", "expert", None, "tensor"),
        P("dp", "expert", "tensor", None),
        P("tensor", None),
        P(),
        P(),
        P("expert", None, None),
        P("dp"),
        P(),
    )
    return jax.shard_map(
        functools.partial(per_device, sizes), mesh=mesh, in_specs=placed, out_specs=P("dp"), check_vma=False
    )
```
